8 devices in a mesh: dp: 2 (over z, y), tp: 4 (over x, core).
Axes of the slice: x: 2, y: 2, z: 1, core: 2. Of those that a mesh axis runs over, the one named last changes fastest.
Arguments:
- x_teach: bfloat16 [8, 768, 1024], P('dp', 'tp')
- x_stud: bfloat16 [8, 768, 312], P(('dp', 'tp'))
- w_up_t: bfloat16 [3, 1024, 4096], P(None, None, 'tp')
- w_down_t: bfloat16 [3, 4096, 1024], P(None, 'tp')
- gain_t: float32 [3, 1024], replicated
- head_t: bfloat16 [1024, 30592], P(None, 'tp')
- w_up_s: bfloat16 [1, 312, 1248], replicated
- w_down_s: bfloat16 [1, 1248, 312], replicated
- gain_s: float32 [1, 312], replicated
- proj_s: bfloat16 [1, 312, 1024], replicated
- head_s: bfloat16 [312, 30592], replicated
Outputs:
- output 1: float32 [], replicated
- output 2: float32 [1, 312, 1248], replicated
- output 3: float32 [1, 1248, 312], replicated
- output 4: float32 [1, 312], replicated
- output 5: float32 [1, 312, 1024], replicated
- output 6: float32 [312, 30592], replicated
All inputs are finite; a program needn't handle non-finite values.
Results may differ from the reference program's by a relative error of at most 0.00750906.
Values are sent between devices in bfloat16 or wider.
A program may use at most 1 GiB of HBM per device.

```python
import jax
import jax.numpy as jnp
from jax import lax

BATCH = 8
SEQ_LEN = 768
D_TEACH = 1024
D_STUD = 312
VOCAB_SIZE = 30592
FEAT_LAYERS = 1
TEACH_LAYERS = 3
NORM_EPS = 1e-6


def setup_inputs(seed: int = 0) -> dict:
    rng_keys = jax.random.split(jax.random.key(seed), 11)
    ff_teach = 4 * D_TEACH
    ff_stud = 4 * D_STUD

    def normal_bf16(rng_key, arr_shape, std_scale):
        return (jax.random.normal(rng_key, arr_shape, jnp.float32) * std_scale).astype(jnp.bfloat16)

    return {
        'x_teach': normal_bf16(rng_keys[0], (BATCH, SEQ_LEN, D_TEACH), 1.0),
        'x_stud': normal_bf16(rng_keys[1], (BATCH, SEQ_LEN, D_STUD), 1.0),
        'w_up_t': normal_bf16(rng_keys[2], (TEACH_LAYERS, D_TEACH, ff_teach), D_TEACH ** -0.5),
        'w_down_t': normal_bf16(rng_keys[3], (TEACH_LAYERS, ff_teach, D_TEACH), ff_teach ** -0.5),
        'gain_t': jax.random.uniform(rng_keys[4], (TEACH_LAYERS, D_TEACH), jnp.float32, 0.5, 1.5),
        'head_t': normal_bf16(rng_keys[5], (D_TEACH, VOCAB_SIZE), D_TEACH ** -0.5),
        'w_up_s': normal_bf16(rng_keys[6], (FEAT_LAYERS, D_STUD, ff_stud), D_STUD ** -0.5),
        'w_down_s': normal_bf16(rng_keys[7], (FEAT_LAYERS, ff_stud, D_STUD), ff_stud ** -0.5),
        'gain_s': jax.random.uniform(rng_keys[8], (FEAT_LAYERS, D_STUD), jnp.float32, 0.5, 1.5),
        'proj_s': normal_bf16(rng_keys[9], (FEAT_LAYERS, D_STUD, D_TEACH), D_STUD ** -0.5),
        'head_s': normal_bf16(rng_keys[10], (D_STUD, VOCAB_SIZE), D_STUD ** -0.5),
    }


def rms_norm(values):
    vals32 = values.astype(jnp.float32)
    return vals32 * lax.rsqrt(jnp.mean(vals32 * vals32, axis=-1, keepdims=True) + NORM_EPS)


def as_bf16(values):
    return values.astype(jnp.bfloat16).astype(jnp.float32)


def gelu_tanh(values):
    return jax.nn.gelu(values, approximate=True)


def teacher_tokens(teach_blk, w_up_t, w_down_t, gain_t, head_t):
    per_feat = TEACH_LAYERS // FEAT_LAYERS
    up_groups = w_up_t.reshape(FEAT_LAYERS, per_feat, D_TEACH, 4 * D_TEACH)
    down_groups = w_down_t.reshape(FEAT_LAYERS, per_feat, 4 * D_TEACH, D_TEACH)
    gain_groups = gain_t.reshape(FEAT_LAYERS, per_feat, D_TEACH)

    def one_layer(hidden, layer_w):
        w_up, w_down, gain_row = layer_w
        normed = (rms_norm(hidden) * gain_row).astype(jnp.bfloat16)
        hidden_act = gelu_tanh(jnp.dot(normed, w_up, preferred_element_type=jnp.float32)).astype(jnp.bfloat16)
        layer_out = jnp.dot(hidden_act, w_down, preferred_element_type=jnp.float32).astype(jnp.bfloat16)
        return hidden + layer_out, None

    def one_feature(hidden, group_w):
        hidden, _ = lax.scan(one_layer, hidden, group_w)
        return hidden, hidden

    hidden, features = lax.scan(one_feature, teach_blk, (up_groups, down_groups, gain_groups))
    teach_logits = jnp.dot(rms_norm(hidden).astype(jnp.bfloat16), head_t, preferred_element_type=jnp.float32)
    return features, teach_logits


def student_loss(params, stud_blk, features, teach_logits, feat_coef, kl_coef):
    w_up, w_down, gains, proj, head_w = params

    def one_block(residual, layer_w):
        up_j, down_j, gain_j, proj_j, feat_j = layer_w
        normed = as_bf16(rms_norm(residual) * gain_j)
        hidden_act = as_bf16(gelu_tanh(jnp.dot(normed, up_j, preferred_element_type=jnp.float32)))
        residual = residual + jnp.dot(hidden_act, down_j, preferred_element_type=jnp.float32)
        proj_in = as_bf16(rms_norm(residual))
        feat_err = jnp.dot(proj_in, proj_j, preferred_element_type=jnp.float32) - feat_j.astype(jnp.float32)
        return residual, jnp.sum(feat_err * feat_err)

    residual, err_sums = lax.scan(one_block, stud_blk.astype(jnp.float32), (w_up, w_down, gains, proj, features))
    stud_logits = jnp.dot(as_bf16(rms_norm(residual)), head_w, preferred_element_type=jnp.float32)
    log_teach = jax.nn.log_softmax(teach_logits, axis=-1)
    log_stud = jax.nn.log_softmax(stud_logits, axis=-1)
    kl_sum = jnp.sum(jnp.exp(log_teach) * (log_teach - log_stud))
    return feat_coef * jnp.sum(err_sums) + kl_coef * kl_sum


def reference(x_teach, x_stud, w_up_t, w_down_t, gain_t, head_t, w_up_s, w_down_s, gain_s, proj_s, head_s):
    block_len = 128
    n_tokens = BATCH * SEQ_LEN
    n_blocks = n_tokens // block_len
    teach_blocks = x_teach.reshape(n_blocks, block_len, D_TEACH)
    stud_blocks = x_stud.reshape(n_blocks, block_len, D_STUD)
    params = (w_up_s.astype(jnp.float32), w_down_s.astype(jnp.float32), gain_s.astype(jnp.float32),
              proj_s.astype(jnp.float32), head_s.astype(jnp.float32))
    feat_coef = 1.0 / (FEAT_LAYERS * n_tokens * D_TEACH)
    kl_coef = 1.0 / n_tokens
    loss_and_grad = jax.value_and_grad(student_loss)

    def one_block(scan_carry, token_blks):
        loss_acc, grad_acc = scan_carry
        teach_blk, stud_blk = token_blks
        features, teach_logits = teacher_tokens(teach_blk, w_up_t, w_down_t, gain_t, head_t)
        loss_val, grad_vals = loss_and_grad(params, stud_blk, features, teach_logits, feat_coef, kl_coef)
        return (loss_acc + loss_val, jax.tree.map(jnp.add, grad_acc, grad_vals)), None

    start_carry = (jnp.zeros((), jnp.float32), jax.tree.map(jnp.zeros_like, params))
    (total_loss, grad_vals), _ = lax.scan(one_block, start_carry, (teach_blocks, stud_blocks))
    grad_up, grad_down, grad_gain, grad_proj, grad_head = grad_vals
    return (total_loss, grad_up, grad_down, grad_gain, grad_proj, grad_head)
```

```python
import functools

import jax
import jax.numpy as jnp
from jax import lax
from jax.experimental import pallas as pl
from jax.experimental.pallas import tpu as pltpu
from jax.sharding import PartitionSpec as P

NORM_EPS = 1e-6
NEG = -1e30
LANES = 128

F32, BF16 = jnp.float32, jnp.bfloat16


def rms_parts(values):
    vals32 = values.astype(F32)
    inv_rms = lax.rsqrt(jnp.mean(vals32 * vals32, axis=-1, keepdims=True) + NORM_EPS)
    return vals32 * inv_rms, inv_rms


def rms_back(normed, inv_rms, grad_out):
    return inv_rms * (grad_out - normed * jnp.mean(grad_out * normed, axis=-1, keepdims=True))


def gelu_tanh(values):
    return jax.nn.gelu(values, approximate=True)


def gelu_back(pre_act, grad_out):
    return jax.vjp(gelu_tanh, pre_act)[1](grad_out)[0]


def mm(lhs, rhs):
    return jnp.dot(lhs, rhs, preferred_element_type=F32)


def mm_tn(lhs, rhs):
    return lax.dot_general(lhs, rhs, (((0,), (0,)), ((), ())), preferred_element_type=F32)


def mm_nt(lhs, rhs):
    return lax.dot_general(lhs, rhs, (((1,), (1,)), ((), ())), preferred_element_type=F32)


def swap_core(v):
    return lax.ppermute(v, 'tp', [(i, i ^ 1) for i in range(4)])


def swap_x(v):
    return lax.ppermute(v, 'tp', [(i, i ^ 2) for i in range(4)])


def swap_y(v):
    return lax.ppermute(v, 'dp', [(0, 1), (1, 0)])


def gather_rel(own, cut):
    px, py = swap_x(own), swap_y(own)
    d0, d1 = swap_y(px[:cut]), swap_x(py[cut:])
    return [own, swap_core(own), px, swap_core(px), py, swap_core(py), (d0, d1), (swap_core(d0), swap_core(d1))]


def flip_rel(arr, axis):
    dp, tp = lax.axis_index('dp'), lax.axis_index('tp')
    shape = arr.shape
    arr = arr.reshape(shape[:axis] + (2, 2, 2) + shape[axis + 1:])
    for off, bit in ((0, dp), (1, tp // 2), (2, tp % 2)):
        arr = jnp.where(bit == 1, jnp.flip(arr, axis + off), arr)
    return arr.reshape(shape)


def params(sem, mib=56):
    return pltpu.CompilerParams(dimension_semantics=sem, vmem_limit_bytes=mib * 2**20)


def is_last_owner():
    return jnp.logical_and(lax.axis_index('tp') == 3, lax.axis_index('dp') == 1)


def online_update(z, bias, m_ref, s_ref, off, rows):
    blocks = [z[:, b * LANES:(b + 1) * LANES] for b in range(z.shape[1] // LANES)]
    blocks[0] = blocks[0] + bias
    m_old = m_ref[off:off + rows, :]
    m_new = functools.reduce(jnp.maximum, blocks, m_old)
    tot = s_ref[off:off + rows, :] * jnp.exp(m_old - m_new)
    for blk in blocks:
        tot = tot + jnp.exp(blk - m_new)
    m_ref[off:off + rows, :] = m_new
    s_ref[off:off + rows, :] = tot


def write_stats(m_ref, s_ref, st_ref):
    m_l = m_ref[...]
    m_row = jnp.max(m_l, axis=1, keepdims=True)
    s_row = jnp.sum(s_ref[...] * jnp.exp(m_l - m_row), axis=1, keepdims=True)
    lane = lax.broadcasted_iota(jnp.int32, m_l.shape, 1)
    packed = jnp.where(lane == 0, m_row, jnp.where(lane == 1, s_row, 0.0))
    st_ref[...] = packed.T[:8, :]


def teach_kernel(sizes, has_alias, bias_ref, *refs):
    x_refs, rest = refs[:len(sizes)], refs[len(sizes):]
    head_ref = rest[0]
    zt_ref, st_ref, m_ref, s_ref = rest[2:] if has_alias else rest[1:]
    j = pl.program_id(0)

    @pl.when(j == 0)
    def _():
        m_ref[...] = jnp.full_like(m_ref, NEG)
        s_ref[...] = jnp.zeros_like(s_ref)

    bias = jnp.where(j == 0, bias_ref[0], 0.0)
    off = 0
    for x_ref, rows in zip(x_refs, sizes):
        z = mm(x_ref[...], head_ref[...])
        zt_ref[off:off + rows, :] = z
        online_update(z, bias, m_ref, s_ref, off, rows)
        off += rows

    @pl.when(j == pl.num_programs(0) - 1)
    def _():
        write_stats(m_ref, s_ref, st_ref)


def teach_stats(pieces, head, bias, zt, pair, n_tok, width):
    cols, depth = head.shape[1], head.shape[0]
    sizes = tuple(p.shape[0] for p in pieces)
    rows = sum(sizes)
    in_specs = [pl.BlockSpec(memory_space=pltpu.SMEM)]
    in_specs += [pl.BlockSpec((s, depth), lambda j: (0, 0)) for s in sizes]
    in_specs += [pl.BlockSpec((depth, width), lambda j: (0, j))]
    args = [bias, *pieces, head]
    alias = {}
    if zt is not None:
        in_specs.append(pl.BlockSpec(memory_space=pl.ANY))
        alias = {len(args): 0}
        args.append(zt)
    return pl.pallas_call(
        functools.partial(teach_kernel, sizes, zt is not None),
        grid=(cols // width,),
        in_specs=in_specs,
        out_specs=(pl.BlockSpec((rows, width), lambda j: (pair, j)), pl.BlockSpec((8, rows), lambda j: (0, 0))),
        out_shape=(jax.ShapeDtypeStruct((n_tok, cols), F32), jax.ShapeDtypeStruct((8, rows), F32)),
        scratch_shapes=[pltpu.VMEM((rows, LANES), F32), pltpu.VMEM((rows, LANES), F32)],
        input_output_aliases=alias,
        compiler_params=params(("arbitrary",)),
        cost_estimate=pl.CostEstimate(flops=2 * rows * cols * depth, bytes_accessed=4 * rows * cols + 2 * depth * cols,
                                      transcendentals=rows * cols),
        name="teach_stats",
    )(*args)


def grad_kernel(coef, sub, has_in, zt_ref, x_ref, xt_ref, hs_ref, hst_ref, lse_ref, *rest):
    if has_in:
        ig_in_ref, ig_ref, hg_ref, kl_ref, lg_ref = rest
    else:
        ig_ref, hg_ref, kl_ref, lg_ref = rest
    i = pl.program_id(0)

    @pl.when(i == 0)
    def _():
        hg_ref[...] = jnp.zeros_like(hg_ref)
        kl_ref[...] = jnp.zeros_like(kl_ref)

    lse_t, lse_s = lse_ref[:, 0:1], lse_ref[:, 1:2]
    for c in range(0, hs_ref.shape[1], sub):
        log_s = mm(x_ref[...], hs_ref[:, c:c + sub]) - lse_s
        log_t = zt_ref[:, c:c + sub] - lse_t
        p_t = jnp.exp(log_t)
        lg_ref[:, c:c + sub] = (jnp.exp(log_s) - p_t).astype(BF16)
        kl_ref[0:1, c:c + sub] += jnp.sum(p_t * (log_t - log_s), axis=0, keepdims=True)
    lg = lg_ref[...]
    hg_ref[...] += mm(xt_ref[...], lg)
    part = mm(lg, hst_ref[...])
    ig_ref[...] = ig_in_ref[...] + part if has_in else part

    @pl.when(i == pl.num_programs(0) - 1)
    def _():
        hg_ref[...] = hg_ref[...] * coef


def grad_pass(zt, x, xt, hs, hst, lse, ig, k, width, rows, coef, sub=256):
    n_tok, depth = x.shape
    in_specs = [pl.BlockSpec((rows, width), lambda i: (i, k)), pl.BlockSpec((rows, depth), lambda i: (i, 0)),
                pl.BlockSpec((depth, rows), lambda i: (0, i)), pl.BlockSpec((depth, width), lambda i: (0, k)),
                pl.BlockSpec((width, depth), lambda i: (k, 0)), pl.BlockSpec((rows, LANES), lambda i: (i, 0))]
    args = [zt, x, xt, hs, hst, lse]
    alias = {}
    if ig is not None:
        in_specs.append(pl.BlockSpec((rows, depth), lambda i: (i, 0)))
        alias = {len(args): 0}
        args.append(ig)
    return pl.pallas_call(
        functools.partial(grad_kernel, coef, sub, ig is not None),
        grid=(n_tok // rows,),
        in_specs=in_specs,
        out_specs=(pl.BlockSpec((rows, depth), lambda i: (i, 0)), pl.BlockSpec((depth, width), lambda i: (0, 0)),
                   pl.BlockSpec((8, width), lambda i: (0, 0))),
        out_shape=(jax.ShapeDtypeStruct((n_tok, depth), F32), jax.ShapeDtypeStruct((depth, width), F32),
                   jax.ShapeDtypeStruct((8, width), F32)),
        scratch_shapes=[pltpu.VMEM((rows, width), BF16)],
        input_output_aliases=alias,
        compiler_params=params(("arbitrary",)),
        cost_estimate=pl.CostEstimate(flops=3 * 2 * n_tok * width * 512, bytes_accessed=4 * n_tok * (width + 800),
                                      transcendentals=2 * n_tok * width),
        name="grad_pass",
    )(*args)


def place_kernel(k, width, span, last_start, cuts, has_alias, *refs):
    n = len(cuts)
    srcs = refs[:n]
    rest = refs[n + 1:] if has_alias else refs[n:]
    out_ref, bufs, sem_in, sem_out = rest[0], rest[1:1 + n], rest[1 + n], rest[2 + n]
    dp, tp = lax.axis_index('dp'), lax.axis_index('tp')
    for q in range(n):
        pltpu.make_async_copy(srcs[q], bufs[q], sem_in.at[q]).start()
    plans = []
    for q, (rel, row, nrow) in enumerate(cuts):
        dy, dx, dc = rel
        owner_tp = 2 * lax.rem(tp // 2 + dx, 2) + lax.rem(lax.rem(tp, 2) + dc, 2)
        owner = 2 * owner_tp + lax.rem(dp + dy, 2)
        plans.append((q, row, nrow, owner))
    for q, row, nrow, owner in plans:
        pltpu.make_async_copy(srcs[q], bufs[q], sem_in.at[q]).wait()
        skip = LANES if k == 0 else 0

        def normal(act, q=q, row=row, nrow=nrow, owner=owner):
            col = pl.multiple_of(owner * span + k * width, LANES)
            getattr(pltpu.make_async_copy(bufs[q], out_ref.at[pl.ds(row, nrow), pl.ds(col, width)], sem_out.at[q]), act)()

        def last(act, q=q, row=row, nrow=nrow):
            src = bufs[q].at[:, pl.ds(skip, width - skip)]
            dst = out_ref.at[pl.ds(row, nrow), pl.ds(last_start + k * width + skip, width - skip)]
            getattr(pltpu.make_async_copy(src, dst, sem_out.at[q]), act)()

        pl.when(owner != 7)(functools.partial(normal, 'start'))
        pl.when(owner == 7)(functools.partial(last, 'start'))
    for q, row, nrow, owner in plans:
        skip = LANES if k == 0 else 0

        def normal_w(q=q, row=row, nrow=nrow, owner=owner):
            col = pl.multiple_of(owner * span + k * width, LANES)
            pltpu.make_async_copy(bufs[q], out_ref.at[pl.ds(row, nrow), pl.ds(col, width)], sem_out.at[q]).wait()

        def last_w(q=q, row=row, nrow=nrow):
            src = bufs[q].at[:, pl.ds(skip, width - skip)]
            dst = out_ref.at[pl.ds(row, nrow), pl.ds(last_start + k * width + skip, width - skip)]
            pltpu.make_async_copy(src, dst, sem_out.at[q]).wait()

        pl.when(owner != 7)(normal_w)
        pl.when(owner == 7)(last_w)


def place(pieces, out, k, width, span, vocab):
    srcs, cuts = [], []
    for r, piece in enumerate(pieces):
        rel = (r // 4, (r // 2) % 2, r % 2)
        row = 0
        for part in (piece if isinstance(piece, tuple) else (piece,)):
            srcs.append(part)
            cuts.append((rel, row, part.shape[0]))
            row += part.shape[0]
    depth = row
    any_spec = pl.BlockSpec(memory_space=pl.ANY)
    args = list(srcs)
    alias = {}
    if out is not None:
        alias = {len(args): 0}
        args.append(out)
    n = len(srcs)
    return pl.pallas_call(
        functools.partial(place_kernel, k, width, span, vocab - span, cuts, out is not None),
        in_specs=[any_spec] * len(args),
        out_specs=any_spec,
        out_shape=jax.ShapeDtypeStruct((depth, vocab), F32),
        scratch_shapes=[pltpu.VMEM(s.shape, F32) for s in srcs] + [pltpu.SemaphoreType.DMA((n,))] * 2,
        input_output_aliases=alias,
        compiler_params=pltpu.CompilerParams(vmem_limit_bytes=24 * 2**20),
        cost_estimate=pl.CostEstimate(flops=4 * 10**9, bytes_accessed=16 * depth * 8 * width // 2, transcendentals=0),
        name="place",
    )(*args)


def neighbours():
    dp, tp = lax.axis_index('dp'), lax.axis_index('tp')
    return {'tp': lax.rem(tp + 2, 4)}, {'dp': 1 - dp}, {'tp': tp + 1 - 2 * lax.rem(tp, 2)}


def entry_barrier():
    sem = pltpu.get_barrier_semaphore()
    for dev in neighbours():
        pl.semaphore_signal(sem, inc=1, device_id=dev, device_id_type=pl.DeviceIdType.MESH)
    pl.semaphore_wait(sem, 3)


def send(src, dst, sems, idx, dev):
    return pltpu.make_async_remote_copy(src_ref=src, dst_ref=dst, send_sem=sems.at[(0, *idx)], recv_sem=sems.at[(1, *idx)],
                                        device_id=dev, device_id_type=pl.DeviceIdType.MESH)


UNIT = 256


def teacher_kernel(bias_ref, x_ref, gain_ref, hs_ref, wu_ref, wd_ref, rj_ref,
                   hid_ref, fin_ref, st_ref, stud_ref, pu, pd, xu, xd, cxu, cxd, yu, yd, cyu, cyd,
                   lu, ld, n_ref, acc_ref, tile_ref, m_ref, s_ref,
                   p_sem, x_sem, cx_sem, y_sem, cy_sem, r_sem, l_sem, t_sem, o_sem):
    dev_x, dev_y, dev_c = neighbours()
    dp = lax.axis_index('dp')
    n_layers = wu_ref.shape[0]
    rows = x_ref.shape[0]
    half = wu_ref.shape[2] // 2
    cut = rows // 2

    def col0(h):
        return pl.multiple_of(dp * half + h * UNIT, UNIT)

    def x_send(l, h):
        j = 2 * l + h
        return (send(wu_ref.at[l, :, pl.ds(col0(h), UNIT)], xu.at[j], x_sem, (0, j), dev_x),
                send(wd_ref.at[l, pl.ds(col0(h), UNIT), :], xd.at[j], x_sem, (1, j), dev_x))

    def cx_send(j):
        return send(xu.at[j], cxu.at[j], cx_sem, (0, j), dev_c), send(xd.at[j], cxd.at[j], cx_sem, (1, j), dev_c)

    def y_send(j):
        return send(xu.at[j], yu.at[j], y_sem, (0, j), dev_y), send(xd.at[j], yd.at[j], y_sem, (1, j), dev_y)

    def cy_send(j):
        return send(yu.at[j], cyu.at[j], cy_sem, (0, j), dev_c), send(yd.at[j], cyd.at[j], cy_sem, (1, j), dev_c)

    def p_send(l):
        return (send(wu_ref.at[l], pu.at[l], p_sem, (0, l), dev_c), send(wd_ref.at[l], pd.at[l], p_sem, (1, l), dev_c))

    def slot(r, lo=0, n=None):
        return stud_ref.at[pl.ds(r * rows + lo, rows if n is None else n)]

    r_x = send(rj_ref, slot(2), r_sem, (0,), dev_x)
    r_y = send(rj_ref, slot(4), r_sem, (1,), dev_y)
    r_c = send(rj_ref, slot(1), r_sem, (2,), dev_c)
    r_cx = send(slot(2), slot(3), r_sem, (3,), dev_c)
    r_cy = send(slot(4), slot(5), r_sem, (4,), dev_c)
    r_xy = send(slot(2, 0, cut), slot(6, 0, cut), r_sem, (5,), dev_y)
    r_yx = send(slot(4, cut, rows - cut), slot(6, cut, rows - cut), r_sem, (6,), dev_x)
    r_cd = send(slot(6), slot(7), r_sem, (7,), dev_c)
    r_own = pltpu.make_async_copy(rj_ref, slot(0), o_sem)

    entry_barrier()
    r_x.start()
    r_y.start()
    r_c.start()
    r_own.start()
    for t in x_send(0, 0) + p_send(0):
        t.start()

    hid_ref[...] = x_ref[...]
    r_x.wait_recv()
    r_xy.start()
    r_cx.start()
    r_y.wait_recv()
    r_yx.start()
    r_cy.start()
    r_own.wait()

    def relay_x(l, h, part, more):
        j = 2 * l + h
        x = x_send(l, h)[part]
        x.wait_recv()
        y_send(j)[part].start()
        cx_send(j)[part].start()
        x.wait_send()
        if h == 0:
            x_send(l, 1)[part].start()
        else:
            @pl.when(more)
            def _():
                x_send(l + 1, 0)[part].start()

    def relay_y(j, part):
        y_send(j)[part].wait_recv()
        cy_send(j)[part].start()

    def stud_tile(r):
        load = pltpu.make_async_copy(slot(r), tile_ref, t_sem)
        load.start()
        load.wait()
        m_ref[...] = jnp.full_like(m_ref, NEG)
        s_ref[...] = jnp.zeros_like(s_ref)
        width = hs_ref.shape[1] // 5

        @pl.loop(0, 5)
        def _(j):
            z = mm(tile_ref[...], hs_ref[:, pl.ds(pl.multiple_of(j * width, width), width)])
            online_update(z, jnp.where(j == 0, bias_ref[0], 0.0), m_ref, s_ref, 0, rows)

        write_stats(m_ref, s_ref, st_ref.at[r])

    def load_units(pairs):
        copies = []
        for u, (src_u, src_d) in pairs:
            copies.append(pltpu.make_async_copy(src_u, lu.at[u], l_sem.at[0, u]))
            copies.append(pltpu.make_async_copy(src_d, ld.at[u], l_sem.at[1, u]))
        for c in copies:
            c.start()
        for c in copies:
            c.wait()

    def run_units(lo, hi):
        @pl.loop(lo, hi)
        def _(u):
            a = gelu_tanh(mm(n_ref[...], lu[u])).astype(BF16)
            acc_ref[...] += mm(a, ld[u])

    stud_tile(0)
    relay_x(0, 0, 0, True)
    r_xy.wait_recv()
    r_yx.wait_recv()
    r_cd.start()
    r_c.wait_recv()
    r_cx.wait_recv()
    r_cy.wait_recv()
    relay_x(0, 0, 1, True)
    r_cd.wait_recv()
    cols = [pl.ds(q * UNIT, UNIT) for q in range(4)]

    @pl.loop(0, n_layers)
    def _(l):
        j0, j1 = 2 * l, 2 * l + 1
        more = l < n_layers - 1
        n_ref[...] = (rms_parts(hid_ref[...])[0] * gain_ref[l]).astype(BF16)
        acc_ref[...] = jnp.zeros_like(acc_ref)
        load_units([(q, (wu_ref.at[l, :, cols[q]], wd_ref.at[l, cols[q], :])) for q in range(4)])
        run_units(0, 4)

        relay_x(l, 1, 0, more)
        relay_y(j0, 0)

        @pl.when(more)
        def _():
            for t in p_send(l + 1):
                t.start()

        for t in p_send(l) + cx_send(j0):
            t.wait_recv()
        load_units([(4 + q, (pu.at[l, :, cols[q]], pd.at[l, cols[q], :])) for q in range(4)]
                   + [(8, (xu.at[j0], xd.at[j0])), (9, (cxu.at[j0], cxd.at[j0]))])
        run_units(4, 10)

        relay_x(l, 1, 1, more)
        relay_y(j0, 1)
        stud_tile(2 * l + 1)
        for t in cx_send(j1) + cy_send(j0):
            t.wait_recv()
        load_units([(10, (xu.at[j1], xd.at[j1])), (11, (cxu.at[j1], cxd.at[j1])),
                    (12, (yu.at[j0], yd.at[j0])), (13, (cyu.at[j0], cyd.at[j0]))])
        run_units(10, 14)

        @pl.when(more)
        def _():
            relay_x(l + 1, 0, 0, True)

        relay_y(j1, 0)
        stud_tile(2 * l + 2)

        @pl.when(more)
        def _():
            relay_x(l + 1, 0, 1, True)

        relay_y(j1, 1)

        @pl.when(jnp.logical_not(more))
        def _():
            stud_tile(7)

        for t in cy_send(j1):
            t.wait_recv()
        load_units([(14, (yu.at[j1], yd.at[j1])), (15, (cyu.at[j1], cyd.at[j1]))])
        run_units(14, 16)
        hid_ref[...] = hid_ref[...] + acc_ref[...].astype(BF16)

    fin_ref[...] = rms_parts(hid_ref[...])[0].astype(BF16)
    for t in (r_x, r_y, r_c, r_cx, r_cy, r_xy, r_yx, r_cd):
        t.wait_send()

    @pl.loop(0, n_layers)
    def _(l):
        for t in p_send(l):
            t.wait_send()
        for h in range(2):
            j = 2 * l + h
            for t in y_send(j) + cx_send(j) + cy_send(j):
                t.wait_send()


def teacher(x, gain, hs, w_up, w_down, rj, bias):
    rows, depth = x.shape
    n_layers, _, shard = w_up.shape
    d_stud = rj.shape[1]
    n_ch = 2 * n_layers
    any_spec, vmem = pl.BlockSpec(memory_space=pl.ANY), pl.BlockSpec(memory_space=pltpu.VMEM)
    up, down = (n_ch, depth, UNIT), (n_ch, UNIT, depth)
    shapes = [((rows, depth), BF16), ((rows, depth), BF16), ((8, 8, rows), F32), ((8 * rows, d_stud), BF16),
              ((n_layers, depth, shard), BF16), ((n_layers, shard, depth), BF16)]
    shapes += [(s, BF16) for s in (up, down) * 4]
    dma = pltpu.SemaphoreType.DMA
    out = pl.pallas_call(
        teacher_kernel,
        in_specs=[pl.BlockSpec(memory_space=pltpu.SMEM), vmem, vmem, vmem, any_spec, any_spec, any_spec],
        out_specs=[vmem, vmem, vmem] + [any_spec] * (len(shapes) - 3),
        out_shape=[jax.ShapeDtypeStruct(*s) for s in shapes],
        scratch_shapes=[pltpu.VMEM((16, depth, UNIT), BF16), pltpu.VMEM((16, UNIT, depth), BF16),
                        pltpu.VMEM((rows, depth), BF16), pltpu.VMEM((rows, depth), F32), pltpu.VMEM((rows, d_stud), BF16),
                        pltpu.VMEM((rows, LANES), F32), pltpu.VMEM((rows, LANES), F32),
                        dma((2, 2, n_layers))] + [dma((2, 2, n_ch))] * 4
        + [dma((2, 8)), dma((2, 16)), dma, dma],
        compiler_params=pltpu.CompilerParams(collective_id=0, has_side_effects=True, vmem_limit_bytes=58 * 2**20),
        name="teacher",
    )(bias, x, gain, hs, w_up, w_down, rj)
    return out[:4]


def solution(mesh):
    dp_size, tp_size = mesh.shape['dp'], mesh.shape['tp']
    n_dev = dp_size * tp_size

    def local_step(x_teach, x_stud, w_up_t, w_down_t, gain_t, head_t, w_up_s, w_down_s, gain_s, proj_s, head_s):
        dp, tp = lax.axis_index('dp'), lax.axis_index('tp')
        n_b, seq_part, d_teach = x_teach.shape
        own_tok = n_b * seq_part
        n_tok = own_tok * n_dev
        d_stud, vocab = head_s.shape
        n_layers = w_up_t.shape[0]
        seq = x_stud.shape[1]
        blocks = -(-vocab // LANES)
        span = -(-blocks // n_dev) * LANES
        n_chunks = 5
        width = span // n_chunks
        feat_coef = 1.0 / (n_tok * d_teach)
        kl_coef = 1.0 / n_tok

        xs = lax.all_to_all(x_stud, 'tp', 1, 0, tiled=True).reshape(own_tok, d_stud)

        owner = 2 * tp + dp
        last = is_last_owner()
        nxt = lax.ppermute(head_t[:, :LANES], 'tp', [(1, 0), (2, 1), (3, 2)])
        vocab_part = head_t.shape[1]
        col_g = jnp.where(last, vocab - span, owner * span)
        my_head = lax.dynamic_slice_in_dim(jnp.concatenate([head_t, nxt], axis=1), col_g - tp * vocab_part, span, axis=1)
        my_hs = lax.dynamic_slice_in_dim(head_s, pl.multiple_of(col_g, LANES), span, axis=1)
        dup = jnp.where(last, n_dev * span - vocab, 0)
        live = lax.broadcasted_iota(jnp.int32, (span, 1), 0) >= dup
        my_hst = jnp.where(live, my_hs.T, jnp.zeros((), BF16))
        bias = jnp.where(last, NEG, 0.0).astype(F32).reshape(1)

        resid0 = xs.astype(F32)
        norm0, _ = rms_parts(resid0)
        normed_s = (norm0 * gain_s[0]).astype(BF16)
        pre_act = mm(normed_s, w_up_s[0])
        act_s = gelu_tanh(pre_act).astype(BF16)
        norm1, inv1 = rms_parts(resid0 + mm(act_s, w_down_s[0]))
        proj_in = norm1.astype(BF16)

        hidden, final_norm, st_s, stud_full = teacher(x_teach.reshape(own_tok, d_teach), gain_t, my_hs, w_up_t, w_down_t,
                                                      proj_in, bias)
        stud_t = stud_full.T

        pieces = gather_rel(final_norm, own_tok // 2)
        zt = None
        stats = []
        for pair in range(4):
            group = []
            for piece in pieces[2 * pair:2 * pair + 2]:
                group += list(piece) if isinstance(piece, tuple) else [piece]
            zt, st = teach_stats(group, my_head, bias, zt, pair, n_tok, width)
            stats.append(st)
        st_t = jnp.concatenate(stats, axis=1)
        local = jnp.stack([st_t[0].reshape(n_dev, own_tok), st_t[1].reshape(n_dev, own_tok), st_s[:, 0], st_s[:, 1]])
        every = lax.all_gather(flip_rel(local, 1), ('dp', 'tp'), axis=0)
        maxima, sums = every[:, 0::2], every[:, 1::2]
        top = jnp.max(maxima, axis=0)
        lse = top + jnp.log(jnp.sum(sums * jnp.exp(maxima - top), axis=0))
        lse = flip_rel(lse, 1).reshape(2, n_tok)
        lse = jnp.pad(lse.T, ((0, 0), (0, LANES - 2)))

        feat_err = mm(proj_in, proj_s[0]) - hidden.astype(F32)
        err_total = jnp.sum(feat_err * feat_err)
        err_grad = (2.0 * feat_coef * feat_err).astype(BF16)
        proj_grad = mm_tn(proj_in, err_grad)
        out_grad = mm_nt(err_grad, proj_s[0])

        ig, head_grad, kl_rows, gathered = None, None, [], []
        cut = (d_stud // 2 + 7) // 8 * 8
        for k in range(n_chunks):
            ig, hg, kl = grad_pass(zt, stud_full, stud_t, my_hs, my_hst, lse, ig, k, width, own_tok, kl_coef)
            kl_rows.append(kl[0])
            gathered.append(gather_rel(hg, cut))
        live_row = lax.broadcasted_iota(jnp.int32, (span,), 0) >= dup
        kl_local = jnp.sum(jnp.where(live_row, jnp.concatenate(kl_rows), 0.0))

        ig = ig.reshape(2, 2, 2, own_tok, d_stud)
        q = ig[:, :, 0] + swap_core(ig[:, :, 1])
        cut_t = own_tok // 2
        first = q[:, 0, :cut_t] + swap_x(q[:, 1, :cut_t])
        second = q[0, :, cut_t:] + swap_y(q[1, :, cut_t:])
        first = first[0] + swap_y(first[1])
        second = second[0] + swap_x(second[1])
        head_in_grad = kl_coef * jnp.concatenate([first, second], axis=0)

        resid_grad = rms_back(norm1, inv1, out_grad + head_in_grad)
        resid_bf = resid_grad.astype(BF16)
        down_t = mm_tn(resid_bf, act_s)
        pre_grad = gelu_back(pre_act, mm_nt(resid_bf, w_down_s[0])).astype(BF16)
        up_grad = mm_tn(normed_s, pre_grad)
        gain_grad = jnp.sum(mm_nt(pre_grad, w_up_s[0]) * norm0, axis=0)
        loss_local = feat_coef * err_total + kl_coef * kl_local

        d_ff = up_grad.shape[1]
        flat = jnp.concatenate([up_grad, down_t, proj_grad], axis=1)
        flat_w = -(-flat.shape[1] // (4 * LANES)) * 4 * LANES
        flat = jnp.pad(flat, ((0, 0), (0, flat_w - flat.shape[1])))
        extra = jnp.pad(gain_grad, (0, flat_w - d_stud))[None]
        extra2 = jnp.pad(loss_local[None], (0, flat_w - 1))[None]
        flat = jnp.concatenate([flat, extra, extra2, jnp.zeros((6, flat_w), F32)], axis=0)
        core = tp % 2
        hw, qw = flat_w // 2, flat_w // 4
        mine = lax.dynamic_slice_in_dim(flat, core * hw, hw, axis=1)
        mine = mine + swap_core(lax.dynamic_slice_in_dim(flat, (1 - core) * hw, hw, axis=1))
        part_a, part_b = mine[:, :qw], mine[:, qw:]
        part_a, part_b = part_a + swap_x(part_a), part_b + swap_y(part_b)
        part_a, part_b = part_a + swap_y(part_a), part_b + swap_x(part_b)
        mine = jnp.concatenate([part_a, part_b], axis=1)
        theirs = swap_core(mine)
        flat = jnp.where(core == 0, jnp.concatenate([mine, theirs], axis=1), jnp.concatenate([theirs, mine], axis=1))
        grad_up = flat[:d_stud, :d_ff][None]
        grad_down = flat[:d_stud, d_ff:2 * d_ff].T[None]
        grad_proj = flat[:d_stud, 2 * d_ff:2 * d_ff + d_teach][None]
        grad_gain = flat[d_stud, :d_stud][None]
        total_loss = flat[d_stud + 1, 0]

        for k in range(n_chunks):
            head_grad = place(gathered[k], head_grad, k, width, span, vocab)
        return total_loss, grad_up, grad_down, grad_gain, grad_proj, head_grad

    in_specs = (P('dp', 'tp', None), P(('dp', 'tp'), None, None), P(None, None, 'tp'), P(None, 'tp', None),
                P(), P(None, 'tp'), P(), P(), P(), P(), P())
    out_specs = (P(), P(), P(), P(), P(), P())
    return jax.shard_map(local_step, mesh=mesh, in_specs=in_specs, out_specs=out_specs, check_vma=False)
```

```python
import functools

import jax
import jax.numpy as jnp
from jax import lax
from jax.experimental import pallas as pl
from jax.experimental.pallas import tpu as pltpu
from jax.sharding import PartitionSpec as P

NORM_EPS = 1e-6
NEG = -1e30
LANES = 128

F32, BF16 = jnp.float32, jnp.bfloat16


def rms_parts(values, axis=-1):
    vals32 = values.astype(F32)
    inv_rms = lax.rsqrt(jnp.mean(vals32 * vals32, axis=axis, keepdims=True) + NORM_EPS)
    return vals32 * inv_rms, inv_rms


def rms_back(normed, inv_rms, grad_out):
    return inv_rms * (grad_out - normed * jnp.mean(grad_out * normed, axis=-1, keepdims=True))


def gelu_tanh(values):
    return jax.nn.gelu(values, approximate=True)


def gelu_back(pre_act, grad_out):
    return jax.vjp(gelu_tanh, pre_act)[1](grad_out)[0]


def mm(lhs, rhs):
    return jnp.dot(lhs, rhs, preferred_element_type=F32)


def mm_tn(lhs, rhs):
    return lax.dot_general(lhs, rhs, (((0,), (0,)), ((), ())), preferred_element_type=F32)


def mm_nt(lhs, rhs):
    return lax.dot_general(lhs, rhs, (((1,), (1,)), ((), ())), preferred_element_type=F32)


def swap_core(v):
    return lax.ppermute(v, 'tp', [(i, i ^ 1) for i in range(4)])


def swap_x(v):
    return lax.ppermute(v, 'tp', [(i, i ^ 2) for i in range(4)])


def swap_y(v):
    return lax.ppermute(v, 'dp', [(0, 1), (1, 0)])


def gather_rel(own, cut):
    px, py = swap_x(own), swap_y(own)
    d0, d1 = swap_y(px[:cut]), swap_x(py[cut:])
    return [own, swap_core(own), px, swap_core(px), py, swap_core(py), (d0, d1), (swap_core(d0), swap_core(d1))]


def flip_rel(arr, axis):
    dp, tp = lax.axis_index('dp'), lax.axis_index('tp')
    shape = arr.shape
    arr = arr.reshape(shape[:axis] + (2, 2, 2) + shape[axis + 1:])
    for off, bit in ((0, dp), (1, tp // 2), (2, tp % 2)):
        arr = jnp.where(bit == 1, jnp.flip(arr, axis + off), arr)
    return arr.reshape(shape)


def params(sem, mib=56):
    return pltpu.CompilerParams(dimension_semantics=sem, vmem_limit_bytes=mib * 2**20)


def is_last_owner():
    return jnp.logical_and(lax.axis_index('tp') == 3, lax.axis_index('dp') == 1)


def online_update(z, bias, m_ref, s_ref, off, rows):
    blocks = [z[:, b * LANES:(b + 1) * LANES] for b in range(z.shape[1] // LANES)]
    blocks[-1] = blocks[-1] + bias
    m_old = m_ref[off:off + rows, :]
    m_new = functools.reduce(jnp.maximum, blocks, m_old)
    tot = s_ref[off:off + rows, :] * jnp.exp(m_old - m_new)
    for blk in blocks:
        tot = tot + jnp.exp(blk - m_new)
    m_ref[off:off + rows, :] = m_new
    s_ref[off:off + rows, :] = tot


def write_stats(m_ref, s_ref, st_ref):
    m_l = m_ref[...]
    m_row = jnp.max(m_l, axis=1, keepdims=True)
    s_row = jnp.sum(s_ref[...] * jnp.exp(m_l - m_row), axis=1, keepdims=True)
    lane = lax.broadcasted_iota(jnp.int32, m_l.shape, 1)
    packed = jnp.where(lane == 0, m_row, jnp.where(lane == 1, s_row, 0.0))
    st_ref[...] = packed.T[:8, :]


def teach_kernel(sizes, has_alias, bias_ref, *refs):
    x_refs, rest = refs[:len(sizes)], refs[len(sizes):]
    head_ref = rest[0]
    zt_ref, st_ref, m_ref, s_ref = rest[2:] if has_alias else rest[1:]
    j = pl.program_id(0)

    @pl.when(j == 0)
    def _():
        m_ref[...] = jnp.full_like(m_ref, NEG)
        s_ref[...] = jnp.zeros_like(s_ref)

    bias = jnp.where(j == pl.num_programs(0) - 1, bias_ref[0], 0.0)
    off = 0
    for x_ref, rows in zip(x_refs, sizes):
        z = mm(x_ref[...], head_ref[...])
        zt_ref[off:off + rows, :] = z
        zt_ref[off:off + rows, -LANES:] = z[:, -LANES:] + bias
        online_update(z, bias, m_ref, s_ref, off, rows)
        off += rows

    @pl.when(j == pl.num_programs(0) - 1)
    def _():
        write_stats(m_ref, s_ref, st_ref)


def teach_stats(pieces, head, bias, zt, pair, n_tok, width):
    cols, depth = head.shape[1], head.shape[0]
    sizes = tuple(p.shape[0] for p in pieces)
    rows = sum(sizes)
    in_specs = [pl.BlockSpec(memory_space=pltpu.SMEM)]
    in_specs += [pl.BlockSpec((s, depth), lambda j: (0, 0)) for s in sizes]
    in_specs += [pl.BlockSpec((depth, width), lambda j: (0, j))]
    args = [bias, *pieces, head]
    alias = {}
    if zt is not None:
        in_specs.append(pl.BlockSpec(memory_space=pl.ANY))
        alias = {len(args): 0}
        args.append(zt)
    return pl.pallas_call(
        functools.partial(teach_kernel, sizes, zt is not None),
        grid=(cols // width,),
        in_specs=in_specs,
        out_specs=(pl.BlockSpec((rows, width), lambda j: (pair, j)), pl.BlockSpec((8, rows), lambda j: (0, 0))),
        out_shape=(jax.ShapeDtypeStruct((n_tok, cols), F32), jax.ShapeDtypeStruct((8, rows), F32)),
        scratch_shapes=[pltpu.VMEM((rows, LANES), F32), pltpu.VMEM((rows, LANES), F32)],
        input_output_aliases=alias,
        compiler_params=params(("arbitrary",)),
        cost_estimate=pl.CostEstimate(flops=2 * rows * cols * depth, bytes_accessed=4 * rows * cols + 2 * depth * cols,
                                      transcendentals=rows * cols),
        name="teach_stats",
    )(*args)


def neighbours():
    dp, tp = lax.axis_index('dp'), lax.axis_index('tp')
    return {'tp': lax.rem(tp + 2, 4)}, {'dp': 1 - dp}, {'tp': tp + 1 - 2 * lax.rem(tp, 2)}


def entry_barrier():
    sem = pltpu.get_barrier_semaphore()
    for dev in neighbours():
        pl.semaphore_signal(sem, inc=1, device_id=dev, device_id_type=pl.DeviceIdType.MESH)
    pl.semaphore_wait(sem, 3)


def send(src, dst, sems, idx, dev):
    return pltpu.make_async_remote_copy(src_ref=src, dst_ref=dst, send_sem=sems.at[(0, *idx)], recv_sem=sems.at[(1, *idx)],
                                        device_id=dev, device_id_type=pl.DeviceIdType.MESH)


def small_sum(src, mine, theirs_out, theirs, land, parts, sems, devs, core):
    dev_x, dev_y, dev_c = devs
    hw = mine.shape[1]
    qw = hw // 2
    give = send(src(pl.multiple_of((1 - core) * hw, LANES), hw), land, sems, (0,), dev_c)
    qa, qb = mine.at[:, pl.ds(0, qw)], mine.at[:, pl.ds(qw, qw)]
    first = [send(qa, parts.at[0], sems, (1,), dev_x), send(qb, parts.at[1], sems, (2,), dev_y)]
    second = [send(qa, parts.at[2], sems, (3,), dev_y), send(qb, parts.at[3], sems, (4,), dev_x)]
    back = send(mine, theirs, sems, (5,), dev_c)

    def halves():
        give.wait()
        mine[...] = src(pl.multiple_of(core * hw, LANES), hw)[...] + land[...]
        for t in first:
            t.start()

    def quarters():
        for t, q, p in zip(first, (qa, qb), (0, 1)):
            t.wait()
            q[...] += parts[p]
        for t in second:
            t.start()

    def rest():
        for t, q, p in zip(second, (qa, qb), (2, 3)):
            t.wait()
            q[...] += parts[p]
        back.start()

    def last():
        back.wait()
        theirs_out[...] = theirs[...]

    return give.start, halves, quarters, rest, last


def grad_kernel(coef, feat_coef, sub, d_ff, bias_ref, err_ref, zt_ref, x_ref, xt_ref, hs_ref, lse_ref, norm1_ref, inv1_ref,
                outg_ref, act_ref, pre_ref, normed_ref, norm0_ref, wu_ref, wd_ref, pg_ref,
                out_ref, kl_ref, pm_ref, pt_ref, gm_ref, gt_ref,
                hg_ref, ig_ref, lg_ref, lc, lxa, lyb, lya, lxb, pback, pland, pparts, gback, gland, gparts,
                own_sem, fwd_sem, core_sem, rs_sem, loc_sem, ps_sem, gs_sem):
    k, i = pl.program_id(0), pl.program_id(1)
    n_k, n_i = pl.num_programs(0), pl.num_programs(1)
    dev_x, dev_y, dev_c = neighbours()
    dp, tp = lax.axis_index('dp'), lax.axis_index('tp')
    depth, width = hs_ref.shape
    rows = x_ref.shape[0]
    cut = (depth // 2 + 7) // 8 * 8
    half = rows // 2
    tx = lax.rem(tp + 2, 4)
    own, x_own, y_own, d_own = 2 * tp + dp, 2 * tx + dp, 2 * tp + 1 - dp, 2 * tx + 1 - dp

    def region(owner, c, lo=0, n=None):
        col = pl.multiple_of(owner * (width * n_k) + c * width, LANES)
        return out_ref.at[pl.ds(lo, depth if n is None else n), pl.ds(col, width)]

    def copies(c):
        return [send(hg_ref.at[c], region(own, c), own_sem, (q, c), dev) for q, dev in enumerate((dev_x, dev_y, dev_c))]

    def local(c):
        return pltpu.make_async_copy(hg_ref.at[c], region(own, c), loc_sem.at[c])

    def forward(c):
        return (send(region(x_own, c, 0, cut), region(x_own, c, 0, cut), fwd_sem, (0, c), dev_y),
                send(region(y_own, c, cut, depth - cut), region(y_own, c, cut, depth - cut), fwd_sem, (1, c), dev_x))

    def core(c):
        return [send(r, r, core_sem, (q, c), dev_c) for q, r in enumerate(
            (region(x_own, c), region(y_own, c), region(d_own, c, 0, cut), region(d_own, c, cut, depth - cut)))]

    def serve(c):
        for q in range(2):
            copies(c)[q].wait_recv()
            forward(c)[q].start()
            core(c)[q].start()

    def serve_far(c):
        for q in range(2):
            forward(c)[q].wait_recv()
            core(c)[2 + q].start()

    @pl.when(jnp.logical_and(k == 0, i == 0))
    def _():
        entry_barrier()
        kl_ref[...] = jnp.zeros_like(kl_ref)

    devs, me_core = (dev_x, dev_y, dev_c), lax.rem(tp, 2)
    proj_steps = small_sum(lambda col, n: pg_ref.at[:, pl.ds(col, n)], pm_ref, pt_ref, pback, pland, pparts, ps_sem, devs, me_core)
    for at, step in zip((0, 1, 3, 5, 7), proj_steps):
        pl.when(jnp.logical_and(k == 0, i == at))(step)

    tok = pl.ds(pl.multiple_of(i * rows, LANES), rows)
    lse_t, lse_s = lse_ref[:, 0:1], lse_ref[:, 1:2]
    for c in range(0, width, sub):
        z_s = mm(x_ref[...], hs_ref[:, c:c + sub])
        if c + sub == width:
            lane = lax.broadcasted_iota(jnp.int32, (1, sub), 1)
            z_s = z_s + jnp.where(jnp.logical_and(lane >= sub - LANES, k == n_k - 1), bias_ref[0], 0.0)
        log_s = z_s - lse_s
        log_t = zt_ref[:, c:c + sub] - lse_t
        p_t = jnp.exp(log_t)
        lg_ref[:, c:c + sub] = (jnp.exp(log_s) - p_t).astype(BF16)
        kl_ref[0:1, c:c + sub] += jnp.sum(p_t * (log_t - log_s), axis=0, keepdims=True)
    lg = lg_ref[...]
    part_h, part_i = mm(xt_ref[...], lg), mm_nt(hs_ref[...], lg)

    @pl.when(i == 0)
    def _():
        hg_ref[k] = part_h

    @pl.when(i > 0)
    def _():
        hg_ref[k] = hg_ref[k] + part_h

    @pl.when(k == 0)
    def _():
        ig_ref[:, tok] = part_i

    @pl.when(k > 0)
    def _():
        ig_ref[:, tok] += part_i

    @pl.when(i == n_i - 1)
    def _():
        hg_ref[k] = hg_ref[k] * coef
        for t in copies(k):
            t.start()
        local(k).start()

    @pl.when(jnp.logical_and(k == 2, i == 2))
    def _():
        serve(0)

    @pl.when(jnp.logical_and(k == 3, i == 5))
    def _():
        serve(1)

    @pl.when(jnp.logical_and(k == n_k - 1, i == n_i - 1))
    def _():
        def col(r, lo=0, n=rows):
            return ig_ref.at[:, pl.ds(r * rows + lo, n)]

        step0 = [send(col(2 * p + 1), lc.at[p], rs_sem, (p,), dev_c) for p in range(4)]
        step1 = [send(col(4 * d + 2, 0, half), lxa.at[d], rs_sem, (4 + d,), dev_x) for d in range(2)]
        step1 += [send(col(4 + 2 * d, half, half), lyb.at[d], rs_sem, (6 + d,), dev_y) for d in range(2)]
        step2 = [send(col(4, 0, half), lya, rs_sem, (8,), dev_y), send(col(2, half, half), lxb, rs_sem, (9,), dev_x)]
        for t in step0:
            t.start()
        for p in range(4):
            step0[p].wait_recv()
            col(2 * p)[...] += lc[p]
        for t in step1:
            t.start()
        serve_far(0)
        serve(2)
        for t in step1:
            t.wait_recv()
        for d in range(2):
            col(4 * d, 0, half)[...] += lxa[d]
            col(2 * d, half, half)[...] += lyb[d]
        for t in step2:
            t.start()
        serve_far(1)
        serve(3)
        for t in step2:
            t.wait_recv()
        for t in step0 + step1 + step2:
            t.wait_send()
        hig = coef * jnp.concatenate([col(0, 0, half)[...] + lya[...], col(0, half, half)[...] + lxb[...]], axis=1)

        grad_out = outg_ref[...] + hig
        normed1 = norm1_ref[...]
        resid = inv1_ref[...] * (grad_out - normed1 * jnp.mean(grad_out * normed1, axis=0, keepdims=True))
        resid = resid.astype(BF16)
        n_ff = act_ref.shape[0]
        ig_ref[:, n_ff:2 * n_ff] = mm_nt(resid, act_ref[...])
        pre_grad = gelu_back(pre_ref[...], mm(wd_ref[...], resid)).astype(BF16)
        up_grad = mm_nt(normed_ref[...], pre_grad)
        gain = jnp.sum(mm(wu_ref[...], pre_grad) * norm0_ref[...], axis=1, keepdims=True)
        loss = feat_coef * err_ref[0] + coef * jnp.sum(kl_ref[0:1, :])
        lane = lax.broadcasted_iota(jnp.int32, up_grad.shape, 1)
        row0 = lax.broadcasted_iota(jnp.int32, up_grad.shape, 0) == 0
        extra = jnp.where(lane == d_ff, gain, jnp.where(jnp.logical_and(lane == d_ff + 1, row0), loss, 0.0))
        ig_ref[:, :n_ff] = jnp.where(lane < d_ff, up_grad, extra)

        grad_steps = small_sum(lambda col, n: ig_ref.at[:, pl.ds(col, n)], gm_ref, gt_ref, gback, gland, gparts, gs_sem, devs, me_core)
        grad_steps[0]()
        serve(4)
        grad_steps[1]()
        serve_far(2)
        grad_steps[2]()
        serve_far(3)
        grad_steps[3]()
        serve_far(4)
        grad_steps[4]()

        @pl.loop(0, n_k)
        def _(c):
            local(c).wait()
            for t in copies(c):
                t.wait_send()
            copies(c)[2].wait_recv()
            for t in forward(c):
                t.wait_send()
            for t in core(c):
                t.wait()


def grad_pass(zt, x, xt, hs, lse, bias, err, back, n_k, rows, coef, feat_coef, d_ff, n_dev, sub=256):
    n_tok, depth = x.shape
    span = hs.shape[1]
    width = span // n_k
    half = rows // 2
    n_ff, d_proj = back[3].shape[0], back[9].shape[1]
    dma = pltpu.SemaphoreType.DMA
    smem = pl.BlockSpec(memory_space=pltpu.SMEM)

    def whole(shape):
        return pl.BlockSpec(shape, lambda k, i: (0,) * len(shape), pipeline_mode=pl.Buffered(1))

    sums = [(depth, d_proj // 2)] * 2 + [(depth, n_ff)] * 2
    return pl.pallas_call(
        functools.partial(grad_kernel, coef, feat_coef, sub, d_ff),
        grid=(n_k, n_tok // rows),
        in_specs=[smem, smem, pl.BlockSpec((rows, width), lambda k, i: (i, k)),
                  pl.BlockSpec((rows, depth), lambda k, i: (i, 0)), pl.BlockSpec((depth, rows), lambda k, i: (0, i)),
                  pl.BlockSpec((depth, width), lambda k, i: (0, k)), pl.BlockSpec((rows, LANES), lambda k, i: (i, 0))]
        + [whole(v.shape) for v in back],
        out_specs=[pl.BlockSpec(memory_space=pl.ANY), whole((8, width))] + [whole(v) for v in sums],
        out_shape=[jax.ShapeDtypeStruct((depth, n_dev * span), F32), jax.ShapeDtypeStruct((8, width), F32)]
        + [jax.ShapeDtypeStruct(v, F32) for v in sums],
        scratch_shapes=[pltpu.VMEM((n_k, depth, width), F32), pltpu.VMEM((depth, n_tok), F32), pltpu.VMEM((rows, width), BF16),
                        pltpu.VMEM((4, depth, rows), F32), pltpu.VMEM((2, depth, half), F32), pltpu.VMEM((2, depth, half), F32),
                        pltpu.VMEM((depth, half), F32), pltpu.VMEM((depth, half), F32),
                        pltpu.VMEM((depth, d_proj // 2), F32), pltpu.VMEM((depth, d_proj // 2), F32), pltpu.VMEM((4, depth, d_proj // 4), F32),
                        pltpu.VMEM((depth, n_ff), F32), pltpu.VMEM((depth, n_ff), F32), pltpu.VMEM((4, depth, n_ff // 2), F32),
                        dma((2, 3, n_k)), dma((2, 2, n_k)), dma((2, 4, n_k)), dma((2, 10)), dma((n_k,)), dma((2, 6)), dma((2, 6))],
        compiler_params=pltpu.CompilerParams(dimension_semantics=("arbitrary", "arbitrary"), collective_id=1,
                                             has_side_effects=True, vmem_limit_bytes=62 * 2**20),
        name="grad_pass",
    )(bias, err, zt, x, xt, hs, lse, *back)


UNIT = 256


def teacher_kernel(bias_ref, x_ref, gain_ref, hs_ref, wu_ref, wd_ref, rj_ref,
                   hid_ref, fin_ref, st_ref, stud_ref, pu, pd, xu, xd, cxu, cxd, yu, yd, cyu, cyd,
                   lu, ld, n_ref, acc_ref, tile_ref, m_ref, s_ref,
                   p_sem, x_sem, cx_sem, y_sem, cy_sem, r_sem, l_sem, t_sem, o_sem):
    dev_x, dev_y, dev_c = neighbours()
    dp = lax.axis_index('dp')
    n_layers = wu_ref.shape[0]
    rows = x_ref.shape[0]
    half = wu_ref.shape[2] // 2
    cut = rows // 2

    def col0(h):
        return pl.multiple_of(dp * half + h * UNIT, UNIT)

    def x_send(l, h):
        j = 2 * l + h
        return (send(wu_ref.at[l, :, pl.ds(col0(h), UNIT)], xu.at[j], x_sem, (0, j), dev_x),
                send(wd_ref.at[l, pl.ds(col0(h), UNIT), :], xd.at[j], x_sem, (1, j), dev_x))

    def cx_send(j):
        return send(xu.at[j], cxu.at[j], cx_sem, (0, j), dev_c), send(xd.at[j], cxd.at[j], cx_sem, (1, j), dev_c)

    def y_send(j):
        return send(xu.at[j], yu.at[j], y_sem, (0, j), dev_y), send(xd.at[j], yd.at[j], y_sem, (1, j), dev_y)

    def cy_send(j):
        return send(yu.at[j], cyu.at[j], cy_sem, (0, j), dev_c), send(yd.at[j], cyd.at[j], cy_sem, (1, j), dev_c)

    def p_send(l):
        return (send(wu_ref.at[l], pu.at[l], p_sem, (0, l), dev_c), send(wd_ref.at[l], pd.at[l], p_sem, (1, l), dev_c))

    def slot(r, lo=0, n=None):
        return stud_ref.at[pl.ds(r * rows + lo, rows if n is None else n)]

    r_x = send(rj_ref, slot(2), r_sem, (0,), dev_x)
    r_y = send(rj_ref, slot(4), r_sem, (1,), dev_y)
    r_c = send(rj_ref, slot(1), r_sem, (2,), dev_c)
    r_cx = send(slot(2), slot(3), r_sem, (3,), dev_c)
    r_cy = send(slot(4), slot(5), r_sem, (4,), dev_c)
    r_xy = send(slot(2, 0, cut), slot(6, 0, cut), r_sem, (5,), dev_y)
    r_yx = send(slot(4, cut, rows - cut), slot(6, cut, rows - cut), r_sem, (6,), dev_x)
    r_cd = send(slot(6), slot(7), r_sem, (7,), dev_c)
    r_own = pltpu.make_async_copy(rj_ref, slot(0), o_sem)

    entry_barrier()
    r_x.start()
    r_y.start()
    r_c.start()
    r_own.start()
    for t in x_send(0, 0) + p_send(0):
        t.start()

    hid_ref[...] = x_ref[...]
    r_x.wait_recv()
    r_xy.start()
    r_cx.start()
    r_y.wait_recv()
    r_yx.start()
    r_cy.start()
    r_own.wait()

    def x_part(j, part):
        l, h = j // 2, lax.rem(j, 2)
        return x_send(l, h)[part]

    def relay_x(j, part):
        x = x_part(j, part)
        x.wait_recv()
        y_send(j)[part].start()
        cx_send(j)[part].start()
        x.wait_send()

        if part == 0:
            @pl.when(j == 0)
            def _():
                x_part(1, 0).start()
            later = (j + 1, 1)
        else:
            later = (j + 2, 0)

        @pl.when(later[0] < 2 * n_layers)
        def _():
            x_part(*later).start()

    def relay_y(j, part):
        y_send(j)[part].wait_recv()
        cy_send(j)[part].start()

    def stud_tile(r):
        load = pltpu.make_async_copy(slot(r), tile_ref, t_sem)
        load.start()
        load.wait()
        m_ref[...] = jnp.full_like(m_ref, NEG)
        s_ref[...] = jnp.zeros_like(s_ref)
        width = hs_ref.shape[1] // 5

        @pl.loop(0, 5)
        def _(j):
            z = mm(tile_ref[...], hs_ref[:, pl.ds(pl.multiple_of(j * width, width), width)])
            online_update(z, jnp.where(j == 4, bias_ref[0], 0.0), m_ref, s_ref, 0, rows)

        write_stats(m_ref, s_ref, st_ref.at[r])

    def load_units(pairs, act):
        for u, (src_u, src_d) in pairs:
            for c in (pltpu.make_async_copy(src_u, lu.at[u], l_sem.at[0, u]), pltpu.make_async_copy(src_d, ld.at[u], l_sem.at[1, u])):
                getattr(c, act)()

    def run_units(lo, hi):
        @pl.loop(lo, hi, step=2)
        def _(u):
            part = None
            for v in range(2):
                p = mm(gelu_tanh(mm(n_ref[...], lu[u + v])).astype(BF16), ld[u + v])
                part = p if part is None else part + p
            acc_ref[...] += part

    cols = [pl.ds(q * UNIT, UNIT) for q in range(4)]

    def own_units(l):
        return [(q, (wu_ref.at[l, :, cols[q]], wd_ref.at[l, cols[q], :])) for q in range(4)]

    def partner_units(l):
        return [(4 + q, (pu.at[l, :, cols[q]], pd.at[l, cols[q], :])) for q in range(4)]

    load_units(own_units(0), 'start')
    stud_tile(0)
    relay_x(0, 0)
    r_xy.wait_recv()
    r_yx.wait_recv()
    r_cd.start()
    r_c.wait_recv()
    r_cx.wait_recv()
    r_cy.wait_recv()
    relay_x(0, 1)
    r_cd.wait_recv()
    for t in p_send(0):
        t.wait_recv()
    load_units(partner_units(0), 'start')

    @pl.loop(0, n_layers)
    def _(l):
        j0, j1 = 2 * l, 2 * l + 1
        more = l < n_layers - 1

        @pl.when(more)
        def _():
            for t in p_send(l + 1):
                t.start()

        n_ref[...] = (rms_parts(hid_ref[...])[0] * gain_ref[l]).astype(BF16)
        acc_ref[...] = jnp.zeros_like(acc_ref)
        load_units(own_units(l), 'wait')
        run_units(0, 4)

        relay_x(j1, 0)
        relay_y(j0, 0)
        for t in cx_send(j0):
            t.wait_recv()
        chip0 = [(8, (xu.at[j0], xd.at[j0])), (9, (cxu.at[j0], cxd.at[j0]))]
        load_units(chip0, 'start')
        load_units(partner_units(l), 'wait')
        load_units(chip0, 'wait')
        run_units(4, 10)

        relay_x(j1, 1)
        relay_y(j0, 1)
        stud_tile(2 * l + 1)
        for t in cx_send(j1) + cy_send(j0):
            t.wait_recv()
        chip1 = [(10, (xu.at[j1], xd.at[j1])), (11, (cxu.at[j1], cxd.at[j1])),
                 (12, (yu.at[j0], yd.at[j0])), (13, (cyu.at[j0], cyd.at[j0]))]
        load_units(chip1, 'start')

        @pl.when(more)
        def _():
            load_units(own_units(l + 1), 'start')
            for t in p_send(l + 1):
                t.wait_recv()
            load_units(partner_units(l + 1), 'start')
            relay_x(j1 + 1, 0)

        relay_y(j1, 0)
        load_units(chip1, 'wait')
        run_units(10, 14)

        @pl.when(more)
        def _():
            relay_x(j1 + 1, 1)

        stud_tile(2 * l + 2)
        relay_y(j1, 1)

        @pl.when(jnp.logical_not(more))
        def _():
            stud_tile(7)

        for t in cy_send(j1):
            t.wait_recv()
        chip2 = [(14, (yu.at[j1], yd.at[j1])), (15, (cyu.at[j1], cyd.at[j1]))]
        load_units(chip2, 'start')
        load_units(chip2, 'wait')
        run_units(14, 16)
        hid_ref[...] = hid_ref[...] + acc_ref[...].astype(BF16)

    fin_ref[...] = rms_parts(hid_ref[...])[0].astype(BF16)
    for t in (r_x, r_y, r_c, r_cx, r_cy, r_xy, r_yx, r_cd):
        t.wait_send()

    @pl.loop(0, n_layers)
    def _(l):
        for t in p_send(l):
            t.wait_send()
        for h in range(2):
            j = 2 * l + h
            for t in y_send(j) + cx_send(j) + cy_send(j):
                t.wait_send()


def teacher(x, gain, hs, w_up, w_down, rj, bias):
    rows, depth = x.shape
    n_layers, _, shard = w_up.shape
    d_stud = rj.shape[1]
    n_ch = 2 * n_layers
    any_spec, vmem = pl.BlockSpec(memory_space=pl.ANY), pl.BlockSpec(memory_space=pltpu.VMEM)
    up, down = (n_ch, depth, UNIT), (n_ch, UNIT, depth)
    shapes = [((rows, depth), BF16), ((rows, depth), BF16), ((8, 8, rows), F32), ((8 * rows, d_stud), BF16),
              ((n_layers, depth, shard), BF16), ((n_layers, shard, depth), BF16)]
    shapes += [(s, BF16) for s in (up, down) * 4]
    dma = pltpu.SemaphoreType.DMA
    out = pl.pallas_call(
        teacher_kernel,
        in_specs=[pl.BlockSpec(memory_space=pltpu.SMEM), vmem, vmem, vmem, any_spec, any_spec, any_spec],
        out_specs=[vmem, vmem, vmem] + [any_spec] * (len(shapes) - 3),
        out_shape=[jax.ShapeDtypeStruct(*s) for s in shapes],
        scratch_shapes=[pltpu.VMEM((16, depth, UNIT), BF16), pltpu.VMEM((16, UNIT, depth), BF16),
                        pltpu.VMEM((rows, depth), BF16), pltpu.VMEM((rows, depth), F32), pltpu.VMEM((rows, d_stud), BF16),
                        pltpu.VMEM((rows, LANES), F32), pltpu.VMEM((rows, LANES), F32),
                        dma((2, 2, n_layers))] + [dma((2, 2, n_ch))] * 4
        + [dma((2, 8)), dma((2, 16)), dma, dma],
        compiler_params=pltpu.CompilerParams(collective_id=0, has_side_effects=True, vmem_limit_bytes=58 * 2**20),
        name="teacher",
    )(bias, x, gain, hs, w_up, w_down, rj)
    return out[:4]


def solution(mesh):
    dp_size, tp_size = mesh.shape['dp'], mesh.shape['tp']
    n_dev = dp_size * tp_size

    def local_step(x_teach, x_stud, w_up_t, w_down_t, gain_t, head_t, w_up_s, w_down_s, gain_s, proj_s, head_s):
        dp, tp = lax.axis_index('dp'), lax.axis_index('tp')
        n_b, seq_part, d_teach = x_teach.shape
        own_tok = n_b * seq_part
        n_tok = own_tok * n_dev
        d_stud, vocab = head_s.shape
        n_layers = w_up_t.shape[0]
        seq = x_stud.shape[1]
        blocks = -(-vocab // LANES)
        span = -(-blocks // n_dev) * LANES
        n_chunks = 5
        width = span // n_chunks
        feat_coef = 1.0 / (n_tok * d_teach)
        kl_coef = 1.0 / n_tok

        xs = lax.all_to_all(x_stud, 'tp', 1, 0, tiled=True).reshape(own_tok, d_stud)

        owner = 2 * tp + dp
        last = is_last_owner()
        nxt = lax.ppermute(head_t[:, :LANES], 'tp', [(1, 0), (2, 1), (3, 2)])
        vocab_part = head_t.shape[1]
        my_head = lax.dynamic_slice_in_dim(jnp.concatenate([head_t, nxt], axis=1), owner * span - tp * vocab_part, span, axis=1)
        over = n_dev * span - vocab
        my_hs = lax.dynamic_slice_in_dim(head_s, pl.multiple_of(owner * span - jnp.where(last, over, 0), LANES), span, axis=1)
        my_hs = jnp.where(last, jnp.pad(my_hs[:, over:], ((0, 0), (0, over))), my_hs)
        bias = jnp.where(last, NEG, 0.0).astype(F32).reshape(1)

        d_ff = w_up_s.shape[2]
        pad_ff = -d_ff % LANES
        up_s = jnp.pad(w_up_s[0], ((0, 0), (0, pad_ff)))
        down_s = jnp.pad(w_down_s[0], ((0, pad_ff), (0, 0)))
        resid0 = xs.T.astype(F32)
        norm0, _ = rms_parts(resid0, 0)
        normed_s = (norm0 * gain_s[0][:, None]).astype(BF16)
        pre_act = mm_tn(up_s, normed_s)
        act_s = gelu_tanh(pre_act).astype(BF16)
        norm1, inv1 = rms_parts(resid0 + mm_tn(down_s, act_s), 0)
        proj_in = norm1.T.astype(BF16)

        hidden, final_norm, st_s, stud_full = teacher(x_teach.reshape(own_tok, d_teach), gain_t, my_hs, w_up_t, w_down_t,
                                                      proj_in, bias)
        stud_t = stud_full.T

        pieces = gather_rel(final_norm, own_tok // 2)
        zt = None
        stats = []
        for pair in range(4):
            group = []
            for piece in pieces[2 * pair:2 * pair + 2]:
                group += list(piece) if isinstance(piece, tuple) else [piece]
            zt, st = teach_stats(group, my_head, bias, zt, pair, n_tok, width)
            stats.append(st)
        st_t = jnp.concatenate(stats, axis=1)
        local = jnp.stack([st_t[0].reshape(n_dev, own_tok), st_t[1].reshape(n_dev, own_tok), st_s[:, 0], st_s[:, 1]])
        every = lax.all_gather(flip_rel(local, 1), ('dp', 'tp'), axis=0)
        maxima, sums = every[:, 0::2], every[:, 1::2]
        top = jnp.max(maxima, axis=0)
        lse = top + jnp.log(jnp.sum(sums * jnp.exp(maxima - top), axis=0))
        lse = flip_rel(lse, 1).reshape(2, n_tok)
        lse = jnp.pad(lse.T, ((0, 0), (0, LANES - 2)))

        feat_err = mm(proj_in, proj_s[0]) - hidden.astype(F32)
        err_total = jnp.sum(feat_err * feat_err)
        err_grad = (2.0 * feat_coef * feat_err).astype(BF16)
        proj_grad = mm_tn(proj_in, err_grad)
        out_grad = mm_nt(proj_s[0], err_grad)

        back = (norm1, inv1, out_grad, act_s, pre_act, normed_s, norm0, up_s, down_s, proj_grad)
        head_grad, _, proj_a, proj_b, ff_a, ff_b = grad_pass(
            zt, stud_full, stud_t, my_hs, lse, bias, err_total.reshape(1), back, n_chunks, own_tok, kl_coef, feat_coef, d_ff, n_dev)
        low = tp % 2 == 0
        grad_proj = jnp.where(low, jnp.concatenate([proj_a, proj_b], axis=1), jnp.concatenate([proj_b, proj_a], axis=1))[None]
        first, second = jnp.where(low, ff_a, ff_b), jnp.where(low, ff_b, ff_a)
        grad_up = first[:, :d_ff][None]
        grad_gain = first[:, d_ff][None]
        total_loss = first[0, d_ff + 1]
        grad_down = second[:, :d_ff].T[None]
        head_grad = head_grad[:, :vocab]
        return total_loss, grad_up, grad_down, grad_gain, grad_proj, head_grad

    in_specs = (P('dp', 'tp', None), P(('dp', 'tp'), None, None), P(None, None, 'tp'), P(None, 'tp', None),
                P(), P(None, 'tp'), P(), P(), P(), P(), P())
    out_specs = (P(), P(), P(), P(), P(), P())
    return jax.shard_map(local_step, mesh=mesh, in_specs=in_specs, out_specs=out_specs, check_vma=False)
```

```python
import functools

import jax
import jax.numpy as jnp
from jax import lax
from jax.experimental import pallas as pl
from jax.experimental.pallas import tpu as pltpu
from jax.sharding import PartitionSpec as P

NORM_EPS = 1e-6
NEG = -1e30
LANES = 128

F32, BF16 = jnp.float32, jnp.bfloat16


def rms_parts(values, axis=-1):
    vals32 = values.astype(F32)
    inv_rms = lax.rsqrt(jnp.mean(vals32 * vals32, axis=axis, keepdims=True) + NORM_EPS)
    return vals32 * inv_rms, inv_rms


def gelu_tanh(values):
    return jax.nn.gelu(values, approximate=True)


def gelu_back(pre_act, grad_out):
    return jax.vjp(gelu_tanh, pre_act)[1](grad_out)[0]


def mm(lhs, rhs):
    return jnp.dot(lhs, rhs, preferred_element_type=F32)


def mm_tn(lhs, rhs):
    return lax.dot_general(lhs, rhs, (((0,), (0,)), ((), ())), preferred_element_type=F32)


def mm_nt(lhs, rhs):
    return lax.dot_general(lhs, rhs, (((1,), (1,)), ((), ())), preferred_element_type=F32)


def swap_core(v):
    return lax.ppermute(v, 'tp', [(i, i ^ 1) for i in range(4)])


def swap_x(v):
    return lax.ppermute(v, 'tp', [(i, i ^ 2) for i in range(4)])


def swap_y(v):
    return lax.ppermute(v, 'dp', [(0, 1), (1, 0)])


def is_last_owner():
    return jnp.logical_and(lax.axis_index('tp') == 3, lax.axis_index('dp') == 1)


def online_update(z, m_ref, s_ref):
    blocks = [z[:, b * LANES:(b + 1) * LANES] for b in range(z.shape[1] // LANES)]
    m_old = m_ref[...]
    m_new = functools.reduce(jnp.maximum, blocks, m_old)
    tot = s_ref[...] * jnp.exp(m_old - m_new)
    for blk in blocks:
        tot = tot + jnp.exp(blk - m_new)
    m_ref[...] = m_new
    s_ref[...] = tot


def lse_row(m_ref, s_ref):
    m_l = m_ref[...]
    m_row = jnp.max(m_l, axis=1, keepdims=True)
    s_row = jnp.sum(s_ref[...] * jnp.exp(m_l - m_row), axis=1, keepdims=True)
    return jnp.broadcast_to(m_row + jnp.log(s_row), m_l.shape).T[:1, :]


def logit_blocks(x, head_ref, col0, width, bias, last, m_ref, s_ref, z_ref=None, sub=256, by_rows=False):
    for c in range(0, width, sub):
        cols = pl.ds(pl.multiple_of(col0 + c, LANES), sub)
        z = mm_nt(x, head_ref[cols, :]) if by_rows else mm(x, head_ref[:, cols])
        if c + sub == width:
            lane = lax.broadcasted_iota(jnp.int32, (1, sub), 1)
            z = z + jnp.where(jnp.logical_and(lane >= sub - LANES, last), bias, 0.0)
        if z_ref is not None:
            z_ref[:, c:c + sub] = z
        online_update(z, m_ref, s_ref)


def neighbours():
    dp, tp = lax.axis_index('dp'), lax.axis_index('tp')
    return {'tp': lax.rem(tp + 2, 4)}, {'dp': 1 - dp}, {'tp': tp + 1 - 2 * lax.rem(tp, 2)}


def peers():
    dp, tp = lax.axis_index('dp'), lax.axis_index('tp')
    core = lax.rem(tp, 2)
    out = []
    for r in range(1, 8):
        base = lax.rem(tp + 2, 4) if r & 2 else tp
        out.append({'dp': 1 - dp if r & 4 else dp, 'tp': base + 1 - 2 * core if r & 1 else base})
    return out


def entry_barrier(devs):
    sem = pltpu.get_barrier_semaphore()
    for dev in devs:
        pl.semaphore_signal(sem, inc=1, device_id=dev, device_id_type=pl.DeviceIdType.MESH)
    pl.semaphore_wait(sem, len(devs))


def send(src, dst, sems, idx, dev):
    return pltpu.make_async_remote_copy(src_ref=src, dst_ref=dst, send_sem=sems.at[(0, *idx)], recv_sem=sems.at[(1, *idx)],
                                        device_id=dev, device_id_type=pl.DeviceIdType.MESH)


def small_sum(src, mine, theirs_out, theirs, land, parts, sems, devs, core):
    dev_x, dev_y, dev_c = devs
    hw = mine.shape[1]
    qw = hw // 2
    give = send(src(pl.multiple_of((1 - core) * hw, LANES), hw), land, sems, (0,), dev_c)
    qa, qb = mine.at[:, pl.ds(0, qw)], mine.at[:, pl.ds(qw, qw)]
    first = [send(qa, parts.at[0], sems, (1,), dev_x), send(qb, parts.at[1], sems, (2,), dev_y)]
    second = [send(qa, parts.at[2], sems, (3,), dev_y), send(qb, parts.at[3], sems, (4,), dev_x)]
    back = send(mine, theirs, sems, (5,), dev_c)

    def halves():
        give.wait()
        mine[...] = src(pl.multiple_of(core * hw, LANES), hw)[...] + land[...]
        for t in first:
            t.start()

    def quarters():
        for t, q, p in zip(first, (qa, qb), (0, 1)):
            t.wait()
            q[...] += parts[p]
        for t in second:
            t.start()

    def rest():
        for t, q, p in zip(second, (qa, qb), (2, 3)):
            t.wait()
            q[...] += parts[p]
        back.start()

    def last():
        back.wait()
        theirs_out[...] = theirs[...]

    return give.start, halves, quarters, rest, last


def grad_kernel(coef, feat_coef, sub, d_ff, bias_ref, err_ref, zt_ref, x_ref, xt_ref, hs_ref, lse_ref, norm1_ref, inv1_ref,
                outg_ref, act_ref, pre_ref, normed_ref, norm0_ref, wu_ref, wd_ref, pg_ref,
                out_ref, kl_ref, pm_ref, pt_ref, gm_ref, gt_ref,
                hg_ref, ig_ref, lg_ref, lc, lxa, lyb, lya, lxb, pback, pland, pparts, gback, gland, gparts,
                own_sem, fwd_sem, core_sem, rs_sem, loc_sem, ps_sem, gs_sem):
    k, i = pl.program_id(0), pl.program_id(1)
    n_k, n_i = pl.num_programs(0), pl.num_programs(1)
    dev_x, dev_y, dev_c = neighbours()
    dp, tp = lax.axis_index('dp'), lax.axis_index('tp')
    depth, width = hs_ref.shape
    rows = x_ref.shape[0]
    cut = (depth // 2 + 7) // 8 * 8
    half = rows // 2
    tx = lax.rem(tp + 2, 4)
    own, x_own, y_own, d_own = 2 * tp + dp, 2 * tx + dp, 2 * tp + 1 - dp, 2 * tx + 1 - dp

    def region(owner, c, lo=0, n=None):
        col = pl.multiple_of(owner * (width * n_k) + c * width, LANES)
        return out_ref.at[pl.ds(lo, depth if n is None else n), pl.ds(col, width)]

    def copies(c):
        return [send(hg_ref.at[c], region(own, c), own_sem, (q, c), dev) for q, dev in enumerate((dev_x, dev_y, dev_c))]

    def local(c):
        return pltpu.make_async_copy(hg_ref.at[c], region(own, c), loc_sem.at[c])

    def forward(c):
        return (send(region(x_own, c, 0, cut), region(x_own, c, 0, cut), fwd_sem, (0, c), dev_y),
                send(region(y_own, c, cut, depth - cut), region(y_own, c, cut, depth - cut), fwd_sem, (1, c), dev_x))

    def core(c):
        return [send(r, r, core_sem, (q, c), dev_c) for q, r in enumerate(
            (region(x_own, c), region(y_own, c), region(d_own, c, 0, cut), region(d_own, c, cut, depth - cut)))]

    def serve(c):
        for q in range(2):
            copies(c)[q].wait_recv()
            forward(c)[q].start()
            core(c)[q].start()

    def serve_far(c):
        for q in range(2):
            forward(c)[q].wait_recv()
            core(c)[2 + q].start()

    @pl.when(jnp.logical_and(k == 0, i == 0))
    def _():
        entry_barrier(neighbours())
        kl_ref[...] = jnp.zeros_like(kl_ref)

    devs, me_core = (dev_x, dev_y, dev_c), lax.rem(tp, 2)
    proj_steps = small_sum(lambda col, n: pg_ref.at[:, pl.ds(col, n)], pm_ref, pt_ref, pback, pland, pparts, ps_sem, devs, me_core)
    for at, step in zip((0, 1, 3, 5, 7), proj_steps):
        pl.when(jnp.logical_and(k == 0, i == at))(step)

    tok = pl.ds(pl.multiple_of(i * rows, LANES), rows)
    lse_t, lse_s = lse_ref[:, 0:1], lse_ref[:, 1:2]
    for c in range(0, width, sub):
        z_s = mm(x_ref[...], hs_ref[:, c:c + sub])
        if c + sub == width:
            lane = lax.broadcasted_iota(jnp.int32, (1, sub), 1)
            z_s = z_s + jnp.where(jnp.logical_and(lane >= sub - LANES, k == n_k - 1), bias_ref[0], 0.0)
        log_s = z_s - lse_s
        log_t = zt_ref[:, c:c + sub] - lse_t
        p_t = jnp.exp(log_t)
        lg_ref[:, c:c + sub] = (jnp.exp(log_s) - p_t).astype(BF16)
        kl_ref[0:1, c:c + sub] += jnp.sum(p_t * (log_t - log_s), axis=0, keepdims=True)
    lg = lg_ref[...]
    part_h, part_i = mm(xt_ref[...], lg), mm_nt(hs_ref[...], lg)

    @pl.when(i == 0)
    def _():
        hg_ref[k] = part_h

    @pl.when(i > 0)
    def _():
        hg_ref[k] = hg_ref[k] + part_h

    @pl.when(k == 0)
    def _():
        ig_ref[:, tok] = part_i

    @pl.when(k > 0)
    def _():
        ig_ref[:, tok] += part_i

    @pl.when(i == n_i - 1)
    def _():
        hg_ref[k] = hg_ref[k] * coef

    @pl.when(jnp.logical_and(i == n_i - 1, k < n_k - 1))
    def _():
        for t in copies(k):
            t.start()
        local(k).start()

    @pl.when(jnp.logical_and(k == 2, i == 2))
    def _():
        serve(0)

    @pl.when(jnp.logical_and(k == 3, i == 5))
    def _():
        serve(1)

    @pl.when(jnp.logical_and(k == n_k - 1, i == n_i - 1))
    def _():
        def col(r, lo=0, n=rows):
            return ig_ref.at[:, pl.ds(r * rows + lo, n)]

        step0 = [send(col(2 * p + 1), lc.at[p], rs_sem, (p,), dev_c) for p in range(4)]
        step1 = [send(col(4 * d + 2, 0, half), lxa.at[d], rs_sem, (4 + d,), dev_x) for d in range(2)]
        step1 += [send(col(4 + 2 * d, half, half), lyb.at[d], rs_sem, (6 + d,), dev_y) for d in range(2)]
        step2 = [send(col(4, 0, half), lya, rs_sem, (8,), dev_y), send(col(2, half, half), lxb, rs_sem, (9,), dev_x)]
        for t in step0:
            t.start()
        serve(2)
        for p in range(4):
            step0[p].wait_recv()
            col(2 * p)[...] += lc[p]
        for t in step1:
            t.start()
        serve_far(0)
        for t in step1:
            t.wait_recv()
        for d in range(2):
            col(4 * d, 0, half)[...] += lxa[d]
            col(2 * d, half, half)[...] += lyb[d]
        for t in step2:
            t.start()
        for t in copies(4):
            t.start()
        local(4).start()
        serve_far(1)
        serve(3)
        for t in step2:
            t.wait_recv()
        for t in step0 + step1 + step2:
            t.wait_send()
        hig = coef * jnp.concatenate([col(0, 0, half)[...] + lya[...], col(0, half, half)[...] + lxb[...]], axis=1)

        grad_out = outg_ref[...] + hig
        normed1 = norm1_ref[...]
        resid = inv1_ref[...] * (grad_out - normed1 * jnp.mean(grad_out * normed1, axis=0, keepdims=True))
        resid = resid.astype(BF16)
        n_ff = act_ref.shape[0]
        ig_ref[:, n_ff:2 * n_ff] = mm_nt(resid, act_ref[...])
        pre_grad = gelu_back(pre_ref[...], mm(wd_ref[...], resid)).astype(BF16)
        up_grad = mm_nt(normed_ref[...], pre_grad)
        gain = jnp.sum(mm(wu_ref[...], pre_grad) * norm0_ref[...], axis=1, keepdims=True)
        loss = feat_coef * err_ref[0] + coef * jnp.sum(kl_ref[0:1, :])
        lane = lax.broadcasted_iota(jnp.int32, up_grad.shape, 1)
        row0 = lax.broadcasted_iota(jnp.int32, up_grad.shape, 0) == 0
        extra = jnp.where(lane == d_ff, gain, jnp.where(jnp.logical_and(lane == d_ff + 1, row0), loss, 0.0))
        ig_ref[:, :n_ff] = jnp.where(lane < d_ff, up_grad, extra)

        grad_steps = small_sum(lambda col, n: ig_ref.at[:, pl.ds(col, n)], gm_ref, gt_ref, gback, gland, gparts, gs_sem, devs, me_core)
        grad_steps[0]()
        serve(4)
        grad_steps[1]()
        serve_far(2)
        grad_steps[2]()
        serve_far(3)
        grad_steps[3]()
        serve_far(4)
        grad_steps[4]()

        @pl.loop(0, n_k)
        def _(c):
            local(c).wait()
            for t in copies(c):
                t.wait_send()
            copies(c)[2].wait_recv()
            for t in forward(c):
                t.wait_send()
            for t in core(c):
                t.wait()


def grad_pass(zt, x, xt, hs, lse, bias, err, back, n_k, rows, coef, feat_coef, d_ff, n_dev, sub=256):
    n_tok, depth = x.shape
    span = hs.shape[1]
    width = span // n_k
    half = rows // 2
    n_ff, d_proj = back[3].shape[0], back[9].shape[1]
    dma = pltpu.SemaphoreType.DMA
    smem = pl.BlockSpec(memory_space=pltpu.SMEM)

    def whole(shape):
        return pl.BlockSpec(shape, lambda k, i: (0,) * len(shape), pipeline_mode=pl.Buffered(1))

    sums = [(depth, d_proj // 2)] * 2 + [(depth, n_ff)] * 2
    return pl.pallas_call(
        functools.partial(grad_kernel, coef, feat_coef, sub, d_ff),
        grid=(n_k, n_tok // rows),
        in_specs=[smem, smem, pl.BlockSpec((rows, width), lambda k, i: (i, k)),
                  pl.BlockSpec((rows, depth), lambda k, i: (i, 0)), pl.BlockSpec((depth, rows), lambda k, i: (0, i)),
                  pl.BlockSpec((depth, width), lambda k, i: (0, k)), pl.BlockSpec((rows, LANES), lambda k, i: (i, 0))]
        + [whole(v.shape) for v in back],
        out_specs=[pl.BlockSpec(memory_space=pl.ANY), whole((8, width))] + [whole(v) for v in sums],
        out_shape=[jax.ShapeDtypeStruct((depth, n_dev * span), F32), jax.ShapeDtypeStruct((8, width), F32)]
        + [jax.ShapeDtypeStruct(v, F32) for v in sums],
        scratch_shapes=[pltpu.VMEM((n_k, depth, width), F32), pltpu.VMEM((depth, n_tok), F32), pltpu.VMEM((rows, width), BF16),
                        pltpu.VMEM((4, depth, rows), F32), pltpu.VMEM((2, depth, half), F32), pltpu.VMEM((2, depth, half), F32),
                        pltpu.VMEM((depth, half), F32), pltpu.VMEM((depth, half), F32),
                        pltpu.VMEM((depth, d_proj // 2), F32), pltpu.VMEM((depth, d_proj // 2), F32), pltpu.VMEM((4, depth, d_proj // 4), F32),
                        pltpu.VMEM((depth, n_ff), F32), pltpu.VMEM((depth, n_ff), F32), pltpu.VMEM((4, depth, n_ff // 2), F32),
                        dma((2, 3, n_k)), dma((2, 2, n_k)), dma((2, 4, n_k)), dma((2, 10)), dma((n_k,)), dma((2, 6)), dma((2, 6))],
        compiler_params=pltpu.CompilerParams(dimension_semantics=("arbitrary", "arbitrary"), collective_id=1,
                                             has_side_effects=True, vmem_limit_bytes=62 * 2**20),
        name="grad_pass",
    )(bias, err, zt, x, xt, hs, lse, *back)


UNIT = 256


def teacher_kernel(bias_ref, x_ref, gain_ref, hs_ref, head_ref, tail_ref, wu_ref, wd_ref, rj_ref, xu0, xd0,
                   hid_ref, lse_ref, zt_ref, stud_ref, pu, pd, xu, xd, cxu, cxd, yu, yd, cyu, cyd,
                   lu, ld, n_ref, acc_ref, tile_ref, m_ref, s_ref, mh, sh, w_ref, fl, stage, pk, sl,
                   p_sem, x_sem, cx_sem, y_sem, cy_sem, r_sem, l_sem, t_sem, o_sem, f_sem, z_sem, s_sem, w_sem):
    dev_x, dev_y, dev_c = neighbours()
    dp = lax.axis_index('dp')
    n_layers = wu_ref.shape[0]
    rows = x_ref.shape[0]
    half = wu_ref.shape[2] // 2
    cut = rows // 2

    def col0(h):
        return pl.multiple_of(dp * half + h * UNIT, UNIT)

    def x_send(l, h):
        j = 2 * l + h
        return (send(wu_ref.at[l, :, pl.ds(col0(h), UNIT)], xu.at[j], x_sem, (0, j), dev_x),
                send(wd_ref.at[l, pl.ds(col0(h), UNIT), :], xd.at[j], x_sem, (1, j), dev_x))

    def from_x(j, first):
        return (xu0, xd0) if first else (xu.at[j], xd.at[j])

    def cx_send(j, first=False):
        up, down = from_x(j, first)
        return send(up, cxu.at[j], cx_sem, (0, j), dev_c), send(down, cxd.at[j], cx_sem, (1, j), dev_c)

    def y_send(j, first=False):
        up, down = from_x(j, first)
        return send(up, yu.at[j], y_sem, (0, j), dev_y), send(down, yd.at[j], y_sem, (1, j), dev_y)

    def cy_send(j):
        return send(yu.at[j], cyu.at[j], cy_sem, (0, j), dev_c), send(yd.at[j], cyd.at[j], cy_sem, (1, j), dev_c)

    def p_send(l):
        return (send(wu_ref.at[l], pu.at[l], p_sem, (0, l), dev_c), send(wd_ref.at[l], pd.at[l], p_sem, (1, l), dev_c))

    def slot(r, lo=0, n=None):
        return stud_ref.at[pl.ds(r * rows + lo, rows if n is None else n)]

    r_x = send(rj_ref, slot(2), r_sem, (0,), dev_x)
    r_y = send(rj_ref, slot(4), r_sem, (1,), dev_y)
    r_c = send(rj_ref, slot(1), r_sem, (2,), dev_c)
    r_cx = send(slot(2), slot(3), r_sem, (3,), dev_c)
    r_cy = send(slot(4), slot(5), r_sem, (4,), dev_c)
    r_xy = send(slot(2, 0, cut), slot(6, 0, cut), r_sem, (5,), dev_y)
    r_yx = send(slot(4, cut, rows - cut), slot(6, cut, rows - cut), r_sem, (6,), dev_x)
    r_cd = send(slot(6), slot(7), r_sem, (7,), dev_c)
    r_own = pltpu.make_async_copy(rj_ref, slot(0), o_sem)

    entry_barrier(peers())
    r_x.start()
    r_y.start()
    r_c.start()
    r_own.start()
    for t in y_send(0, True) + cx_send(0, True) + x_send(0, 1) + p_send(0):
        t.start()
    x_send(1, 0)[0].start()

    tp = lax.axis_index('tp')
    shard, span = head_ref.shape[0], w_ref.shape[0]
    shift = pl.multiple_of(tp * (-shard % LANES), -shard % LANES)
    n_in = shard // LANES * LANES - span
    w_first = pltpu.make_async_copy(head_ref.at[pl.ds(shift, span)], w_ref, w_sem.at[0])
    w_second = (pltpu.make_async_copy(head_ref.at[pl.ds(span + shift, n_in)], w_ref.at[pl.ds(0, n_in)], w_sem.at[0]),
                pltpu.make_async_copy(tail_ref.at[pl.ds(shift, span - n_in)], w_ref.at[pl.ds(n_in, span - n_in)], w_sem.at[1]))

    def load_head(act):
        @pl.when(dp == 0)
        def _():
            getattr(w_first, act)()

        @pl.when(dp == 1)
        def _():
            for c in w_second:
                getattr(c, act)()

    load_head('start')
    hid_ref[...] = x_ref[...]
    r_x.wait_recv()
    r_xy.start()
    r_cx.start()
    r_y.wait_recv()
    r_yx.start()
    r_cy.start()
    r_own.wait()

    def x_part(j, part):
        l, h = j // 2, lax.rem(j, 2)
        return x_send(l, h)[part]

    def relay_x(j, part):
        x = x_part(j, part)
        x.wait_recv()
        y_send(j)[part].start()
        cx_send(j)[part].start()
        x.wait_send()

        later = (j + 1, 1) if part == 0 else (j + 2, 0)

        @pl.when(later[0] < 2 * n_layers)
        def _():
            x_part(*later).start()

    def relay_y(j, part):
        y_send(j)[part].wait_recv()
        cy_send(j)[part].start()

    n_col = 5
    width = hs_ref.shape[1] // n_col

    def stud_tile(r):
        load = pltpu.make_async_copy(slot(r), tile_ref, t_sem)
        load.start()
        load.wait()
        m_ref[...] = jnp.full_like(m_ref, NEG)
        s_ref[...] = jnp.zeros_like(s_ref)

        @pl.loop(0, n_col)
        def _(j):
            logit_blocks(tile_ref[...], hs_ref, j * width, width, bias_ref[0], j == n_col - 1, m_ref, s_ref)

        pk[pl.ds(8 + r, 1), :] = lse_row(m_ref, s_ref)

    def load_units(pairs, act):
        for u, (src_u, src_d) in pairs:
            for c in (pltpu.make_async_copy(src_u, lu.at[u], l_sem.at[0, u]), pltpu.make_async_copy(src_d, ld.at[u], l_sem.at[1, u])):
                getattr(c, act)()

    def run_units(lo, hi):
        @pl.loop(lo, hi, step=2)
        def _(u):
            part = None
            for v in range(2):
                p = mm(gelu_tanh(mm(n_ref[...], lu[u + v])).astype(BF16), ld[u + v])
                part = p if part is None else part + p
            acc_ref[...] += part

    cols = [pl.ds(q * UNIT, UNIT) for q in range(4)]

    def own_units(l):
        return [(q, (wu_ref.at[l, :, cols[q]], wd_ref.at[l, cols[q], :])) for q in range(4)]

    def partner_units(l):
        return [(4 + q, (pu.at[l, :, cols[q]], pd.at[l, cols[q], :])) for q in range(4)]

    load_units(own_units(0), 'start')
    stud_tile(0)
    r_xy.wait_recv()
    r_yx.wait_recv()
    r_cd.start()
    r_c.wait_recv()
    r_cx.wait_recv()
    r_cy.wait_recv()
    r_cd.wait_recv()
    for t in p_send(0):
        t.wait_recv()
    load_units(partner_units(0), 'start')

    @pl.loop(0, n_layers)
    def _(l):
        j0, j1 = 2 * l, 2 * l + 1
        more = l < n_layers - 1

        @pl.when(more)
        def _():
            for t in p_send(l + 1):
                t.start()

        n_ref[...] = (rms_parts(hid_ref[...])[0] * gain_ref[l]).astype(BF16)
        acc_ref[...] = jnp.zeros_like(acc_ref)
        load_units(own_units(l), 'wait')
        run_units(0, 4)

        relay_x(j1, 0)
        relay_y(j0, 0)
        for t in cx_send(j0):
            t.wait_recv()
        chip0 = [(8, from_x(j0, False)), (9, (cxu.at[j0], cxd.at[j0]))]

        @pl.when(l == 0)
        def _():
            load_units([(8, from_x(j0, True))], 'start')

        @pl.when(l > 0)
        def _():
            load_units(chip0[:1], 'start')

        load_units(chip0[1:], 'start')
        load_units(partner_units(l), 'wait')
        load_units(chip0, 'wait')
        run_units(4, 10)

        relay_x(j1, 1)
        relay_y(j0, 1)
        stud_tile(2 * l + 1)
        for t in cx_send(j1) + cy_send(j0):
            t.wait_recv()
        chip1 = [(10, (xu.at[j1], xd.at[j1])), (11, (cxu.at[j1], cxd.at[j1])),
                 (12, (yu.at[j0], yd.at[j0])), (13, (cyu.at[j0], cyd.at[j0]))]
        load_units(chip1, 'start')

        @pl.when(more)
        def _():
            load_units(own_units(l + 1), 'start')
            for t in p_send(l + 1):
                t.wait_recv()
            load_units(partner_units(l + 1), 'start')
            relay_x(j1 + 1, 0)

        relay_y(j1, 0)
        load_units(chip1, 'wait')
        run_units(10, 14)

        @pl.when(more)
        def _():
            relay_x(j1 + 1, 1)

        stud_tile(2 * l + 2)
        relay_y(j1, 1)

        @pl.when(jnp.logical_not(more))
        def _():
            stud_tile(7)

        for t in cy_send(j1):
            t.wait_recv()
        chip2 = [(14, (yu.at[j1], yd.at[j1])), (15, (cyu.at[j1], cyd.at[j1]))]
        load_units(chip2, 'start')
        load_units(chip2, 'wait')
        run_units(14, 16)
        hid_ref[...] = hid_ref[...] + acc_ref[...].astype(BF16)

    fl[0] = rms_parts(hid_ref[...])[0].astype(BF16)
    load_head('wait')

    def part(r, h):
        return fl.at[r, pl.ds(h * cut, cut)]

    f_x = [send(part(0, h), part(2, h), f_sem, (h,), dev_x) for h in range(2)]
    f_y = [send(part(0, h), part(4, h), f_sem, (2 + h,), dev_y) for h in range(2)]
    f_c = send(fl.at[0], fl.at[1], f_sem, (4,), dev_c)
    f_cx = [send(part(2, h), part(3, h), f_sem, (5 + h,), dev_c) for h in range(2)]
    f_cy = [send(part(4, h), part(5, h), f_sem, (7 + h,), dev_c) for h in range(2)]
    f_d = [send(part(2, 0), part(6, 0), f_sem, (9,), dev_y), send(part(4, 1), part(6, 1), f_sem, (10,), dev_x)]
    f_cd = [send(part(6, h), part(7, h), f_sem, (11 + h,), dev_c) for h in range(2)]
    for t in (f_x[0], f_y[1], f_c):
        t.start()

    def on_arrival(g, arrived, then):
        @pl.when(g == then[0])
        def _():
            for t in arrived:
                t.wait_recv()
            for t in then[1]:
                t.start()

    @pl.loop(0, 8)
    def _(g):
        on_arrival(g, [f_c], (1, []))
        on_arrival(g, [f_x[0], f_y[1]], (2, [f_cx[0], f_cy[1], f_x[1], f_y[0]]))
        on_arrival(g, [f_cx[0], f_cy[1]], (3, []))
        on_arrival(g, [f_x[1], f_y[0]], (4, [f_d[0], f_d[1], f_cx[1], f_cy[0]]))
        on_arrival(g, [f_cx[1], f_cy[0]], (5, []))
        on_arrival(g, f_d, (6, f_cd))
        on_arrival(g, f_cd, (7, []))
        mixed = jnp.logical_and(g >= 2, g < 6)
        late = jnp.logical_and(g >= 4, g < 6)

        @pl.loop(0, 2)
        def _(u):
            r = g - jnp.where(late, 2, 0) + jnp.where(mixed, 2 * u, 0)
            h = jnp.where(late, 1 - u, u)
            row = pl.multiple_of(h * cut, cut)
            mh[...] = jnp.full_like(mh, NEG)
            sh[...] = jnp.zeros_like(sh)

            @pl.loop(0, n_col)
            def _(j):
                n = (2 * g + u) * n_col + j
                slot_z = lax.rem(n, 2)
                store = pltpu.make_async_copy(stage.at[slot_z], zt_ref.at[pl.ds(pl.multiple_of(r * rows + row, cut), cut),
                                                                          pl.ds(pl.multiple_of(j * width, LANES), width)],
                                              z_sem.at[slot_z])

                @pl.when(n >= 2)
                def _():
                    store.wait()

                logit_blocks(fl[r, pl.ds(row, cut), :], w_ref, j * width, width, bias_ref[0], j == n_col - 1, mh, sh,
                             stage.at[slot_z], by_rows=True)
                store.start()

            pk[pl.ds(r, 1), pl.ds(row, cut)] = lse_row(mh, sh)

    for q in range(2):
        pltpu.make_async_copy(stage.at[q], zt_ref.at[pl.ds(0, cut), pl.ds(0, width)], z_sem.at[q]).wait()

    tell = [send(pk, sl.at[r], s_sem, (r,), dev) for r, dev in zip(range(1, 8), peers())]
    for t in tell:
        t.start()
    sl[0] = pk[...]
    for t in tell:
        t.wait_recv()
    sub = lax.broadcasted_iota(jnp.int32, (LANES, 1), 0)
    for q in range(8):
        both = []
        for base in (0, 8):
            vals = [sl[r, base + (q ^ r):base + (q ^ r) + 1, :] for r in range(8)]
            top = functools.reduce(jnp.maximum, vals)
            both.append(top + jnp.log(sum(jnp.exp(v - top) for v in vals)))
        lse_ref[q * rows:(q + 1) * rows, :] = jnp.where(sub == 0, both[0], jnp.where(sub == 1, both[1], 0.0)).T
    for t in tell + f_x + f_y + f_cx + f_cy + f_d + f_cd + [f_c]:
        t.wait_send()

    for t in (r_x, r_y, r_c, r_cx, r_cy, r_xy, r_yx, r_cd):
        t.wait_send()

    @pl.loop(0, n_layers)
    def _(l):
        for t in p_send(l):
            t.wait_send()
        for h in range(2):
            j = 2 * l + h
            for t in y_send(j) + cx_send(j) + cy_send(j):
                t.wait_send()


def teacher(x, gain, hs, head, tail, w_up, w_down, rj, bias, ahead):
    rows, depth = x.shape
    n_layers, _, shard = w_up.shape
    d_stud, span = hs.shape
    n_ch, cut = 2 * n_layers, rows // 2
    width = span // 5
    any_spec, vmem = pl.BlockSpec(memory_space=pl.ANY), pl.BlockSpec(memory_space=pltpu.VMEM)
    up, down = (n_ch, depth, UNIT), (n_ch, UNIT, depth)
    shapes = [((rows, depth), BF16), ((8 * rows, LANES), F32), ((8 * rows, span), F32), ((8 * rows, d_stud), BF16),
              ((n_layers, depth, shard), BF16), ((n_layers, shard, depth), BF16)]
    shapes += [(s, BF16) for s in (up, down) * 4]
    dma = pltpu.SemaphoreType.DMA
    out = pl.pallas_call(
        teacher_kernel,
        in_specs=[pl.BlockSpec(memory_space=pltpu.SMEM), vmem, vmem, vmem] + [any_spec] * 7,
        out_specs=[vmem, vmem] + [any_spec] * (len(shapes) - 2),
        out_shape=[jax.ShapeDtypeStruct(*s) for s in shapes],
        scratch_shapes=[pltpu.VMEM((16, depth, UNIT), BF16), pltpu.VMEM((16, UNIT, depth), BF16),
                        pltpu.VMEM((rows, depth), BF16), pltpu.VMEM((rows, depth), F32), pltpu.VMEM((rows, d_stud), BF16),
                        pltpu.VMEM((rows, LANES), F32), pltpu.VMEM((rows, LANES), F32),
                        pltpu.VMEM((cut, LANES), F32), pltpu.VMEM((cut, LANES), F32),
                        pltpu.VMEM((span, depth), BF16), pltpu.VMEM((8, rows, depth), BF16),
                        pltpu.VMEM((2, cut, width), F32), pltpu.VMEM((16, rows), F32), pltpu.VMEM((8, 16, rows), F32),
                        dma((2, 2, n_layers))] + [dma((2, 2, n_ch))] * 4
        + [dma((2, 8)), dma((2, 16)), dma, dma, dma((2, 13)), dma((2,)), dma((2, 8)), dma((2,))],
        compiler_params=pltpu.CompilerParams(collective_id=0, has_side_effects=True, vmem_limit_bytes=63 * 2**20),
        name="teacher",
    )(bias, x, gain, hs, head, tail, w_up, w_down, rj, *ahead)
    return out[:4]


def solution(mesh):
    dp_size, tp_size = mesh.shape['dp'], mesh.shape['tp']
    n_dev = dp_size * tp_size

    def local_step(x_teach, x_stud, w_up_t, w_down_t, gain_t, head_t, w_up_s, w_down_s, gain_s, proj_s, head_s):
        dp, tp = lax.axis_index('dp'), lax.axis_index('tp')
        n_b, seq_part, d_teach = x_teach.shape
        own_tok = n_b * seq_part
        n_tok = own_tok * n_dev
        d_stud, vocab = head_s.shape
        n_layers = w_up_t.shape[0]
        seq = x_stud.shape[1]
        blocks = -(-vocab // LANES)
        span = -(-blocks // n_dev) * LANES
        n_chunks = 5
        width = span // n_chunks
        feat_coef = 1.0 / (n_tok * d_teach)
        kl_coef = 1.0 / n_tok

        first = dp * (w_up_t.shape[2] // 2)
        ahead = (swap_x(lax.dynamic_slice_in_dim(w_up_t[0], first, UNIT, axis=1)),
                 swap_x(lax.dynamic_slice_in_dim(w_down_t[0], first, UNIT, axis=0)))

        def seq_rows(other):
            return lax.dynamic_slice_in_dim(x_stud[0], other * seq_part, seq_part, axis=0)

        from_c = swap_core(seq_rows(tp + 1 - 2 * (tp % 2)))
        from_x = swap_x(seq_rows((tp + 2) % 4))
        from_d = lax.ppermute(seq_rows(3 - tp), 'tp', [(i, 3 - i) for i in range(4)])
        mine = seq_rows(tp)
        odd, right = tp % 2 == 1, tp >= 2
        low, high = jnp.where(odd, from_c, mine), jnp.where(odd, mine, from_c)
        far_low, far_high = jnp.where(odd, from_d, from_x), jnp.where(odd, from_x, from_d)
        xs = jnp.concatenate([jnp.where(right, far_low, low), jnp.where(right, far_high, high),
                              jnp.where(right, low, far_low), jnp.where(right, high, far_high)], axis=0)

        owner = 2 * tp + dp
        last = is_last_owner()
        head_rows = head_t.T
        nxt = lax.ppermute(head_rows[:LANES], 'tp', [(1, 0), (2, 1), (3, 2)])
        edge = head_rows.shape[0] // LANES * LANES
        tail = jnp.concatenate([head_rows[edge:], nxt], axis=0)
        over = n_dev * span - vocab
        my_hs = lax.dynamic_slice_in_dim(head_s, pl.multiple_of(owner * span - jnp.where(last, over, 0), LANES), span, axis=1)
        my_hs = jnp.where(last, jnp.pad(my_hs[:, over:], ((0, 0), (0, over))), my_hs)
        bias = jnp.where(last, NEG, 0.0).astype(F32).reshape(1)

        d_ff = w_up_s.shape[2]
        pad_ff = -d_ff % LANES
        up_s = jnp.pad(w_up_s[0], ((0, 0), (0, pad_ff)))
        down_s = jnp.pad(w_down_s[0], ((0, pad_ff), (0, 0)))
        resid0 = xs.T.astype(F32)
        norm0, _ = rms_parts(resid0, 0)
        normed_s = (norm0 * gain_s[0][:, None]).astype(BF16)
        pre_act = mm_tn(up_s, normed_s)
        act_s = gelu_tanh(pre_act).astype(BF16)
        norm1, inv1 = rms_parts(resid0 + mm_tn(down_s, act_s), 0)
        proj_in = norm1.T.astype(BF16)

        hidden, lse, zt, stud_full = teacher(x_teach.reshape(own_tok, d_teach), gain_t, my_hs, head_rows, tail, w_up_t, w_down_t,
                                             proj_in, bias, ahead)
        stud_t = stud_full.T

        feat_err = mm(proj_in, proj_s[0]) - hidden.astype(F32)
        err_total = jnp.sum(feat_err * feat_err)
        err_grad = (2.0 * feat_coef * feat_err).astype(BF16)
        proj_grad = mm_tn(proj_in, err_grad)
        out_grad = mm_nt(proj_s[0], err_grad)

        back = (norm1, inv1, out_grad, act_s, pre_act, normed_s, norm0, up_s, down_s, proj_grad)
        head_grad, _, proj_a, proj_b, ff_a, ff_b = grad_pass(
            zt, stud_full, stud_t, my_hs, lse, bias, err_total.reshape(1), back, n_chunks, own_tok, kl_coef, feat_coef, d_ff, n_dev)
        low = tp % 2 == 0
        grad_proj = jnp.where(low, jnp.concatenate([proj_a, proj_b], axis=1), jnp.concatenate([proj_b, proj_a], axis=1))[None]
        first, second = jnp.where(low, ff_a, ff_b), jnp.where(low, ff_b, ff_a)
        grad_up = first[:, :d_ff][None]
        grad_gain = first[:, d_ff][None]
        total_loss = first[0, d_ff + 1]
        grad_down = second[:, :d_ff].T[None]
        head_grad = head_grad[:, :vocab]
        return total_loss, grad_up, grad_down, grad_gain, grad_proj, head_grad

    in_specs = (P('dp', 'tp', None), P(('dp', 'tp'), None, None), P(None, None, 'tp'), P(None, 'tp', None),
                P(), P(None, 'tp'), P(), P(), P(), P(), P())
    out_specs = (P(), P(), P(), P(), P(), P())
    return jax.shard_map(local_step, mesh=mesh, in_specs=in_specs, out_specs=out_specs, check_vma=False)
```

```python
import functools

import jax
import jax.numpy as jnp
from jax import lax
from jax.experimental import pallas as pl
from jax.experimental.pallas import tpu as pltpu
from jax.sharding import PartitionSpec as P

NORM_EPS = 1e-6
NEG = -1e30
LANES = 128

F32, BF16 = jnp.float32, jnp.bfloat16


def rms_parts(values, axis=-1):
    vals32 = values.astype(F32)
    inv_rms = lax.rsqrt(jnp.mean(vals32 * vals32, axis=axis, keepdims=True) + NORM_EPS)
    return vals32 * inv_rms, inv_rms


def gelu_tanh(values):
    return jax.nn.gelu(values, approximate=True)


def gelu_back(pre_act, grad_out):
    return jax.vjp(gelu_tanh, pre_act)[1](grad_out)[0]


def mm(lhs, rhs):
    return jnp.dot(lhs, rhs, preferred_element_type=F32)


def mm_tn(lhs, rhs):
    return lax.dot_general(lhs, rhs, (((0,), (0,)), ((), ())), preferred_element_type=F32)


def mm_nt(lhs, rhs):
    return lax.dot_general(lhs, rhs, (((1,), (1,)), ((), ())), preferred_element_type=F32)


def swap_core(v):
    return lax.ppermute(v, 'tp', [(i, i ^ 1) for i in range(4)])


def swap_x(v):
    return lax.ppermute(v, 'tp', [(i, i ^ 2) for i in range(4)])


def swap_y(v):
    return lax.ppermute(v, 'dp', [(0, 1), (1, 0)])


def is_last_owner():
    return jnp.logical_and(lax.axis_index('tp') == 3, lax.axis_index('dp') == 1)


def online_update(z, m_ref, s_ref):
    blocks = [z[:, b * LANES:(b + 1) * LANES] for b in range(z.shape[1] // LANES)]
    m_old = m_ref[...]
    m_new = functools.reduce(jnp.maximum, blocks, m_old)
    tot = s_ref[...] * jnp.exp(m_old - m_new)
    for blk in blocks:
        tot = tot + jnp.exp(blk - m_new)
    m_ref[...] = m_new
    s_ref[...] = tot


def lse_row(m_ref, s_ref):
    m_l = m_ref[...]
    m_row = jnp.max(m_l, axis=1, keepdims=True)
    s_row = jnp.sum(s_ref[...] * jnp.exp(m_l - m_row), axis=1, keepdims=True)
    return jnp.broadcast_to(m_row + jnp.log(s_row), m_l.shape).T[:1, :]


def logit_blocks(x, head_ref, col0, width, bias, last, m_ref, s_ref, z_ref=None, sub=256, by_rows=False):
    for c in range(0, width, sub):
        cols = pl.ds(pl.multiple_of(col0 + c, LANES), sub)
        z = mm_nt(x, head_ref[cols, :]) if by_rows else mm(x, head_ref[:, cols])
        if c + sub == width:
            lane = lax.broadcasted_iota(jnp.int32, (1, sub), 1)
            z = z + jnp.where(jnp.logical_and(lane >= sub - LANES, last), bias, 0.0)
        if z_ref is not None:
            z_ref[:, c:c + sub] = z
        online_update(z, m_ref, s_ref)


def neighbours():
    dp, tp = lax.axis_index('dp'), lax.axis_index('tp')
    return {'tp': lax.rem(tp + 2, 4)}, {'dp': 1 - dp}, {'tp': tp + 1 - 2 * lax.rem(tp, 2)}


def peers():
    dp, tp = lax.axis_index('dp'), lax.axis_index('tp')
    core = lax.rem(tp, 2)
    out = []
    for r in range(1, 8):
        base = lax.rem(tp + 2, 4) if r & 2 else tp
        out.append({'dp': 1 - dp if r & 4 else dp, 'tp': base + 1 - 2 * core if r & 1 else base})
    return out


def entry_barrier(devs):
    sem = pltpu.get_barrier_semaphore()
    for dev in devs:
        pl.semaphore_signal(sem, inc=1, device_id=dev, device_id_type=pl.DeviceIdType.MESH)
    pl.semaphore_wait(sem, len(devs))


def send(src, dst, sems, idx, dev):
    return pltpu.make_async_remote_copy(src_ref=src, dst_ref=dst, send_sem=sems.at[(0, *idx)], recv_sem=sems.at[(1, *idx)],
                                        device_id=dev, device_id_type=pl.DeviceIdType.MESH)


def small_sum(src, mine, theirs_out, theirs, land, parts, sems, devs, core):
    dev_x, dev_y, dev_c = devs
    hw = mine.shape[1]
    qw = hw // 2
    give = send(src(pl.multiple_of((1 - core) * hw, LANES), hw), land, sems, (0,), dev_c)
    qa, qb = mine.at[:, pl.ds(0, qw)], mine.at[:, pl.ds(qw, qw)]
    first = [send(qa, parts.at[0], sems, (1,), dev_x), send(qb, parts.at[1], sems, (2,), dev_y)]
    second = [send(qa, parts.at[2], sems, (3,), dev_y), send(qb, parts.at[3], sems, (4,), dev_x)]
    back = send(mine, theirs, sems, (5,), dev_c)

    def halves():
        give.wait()
        mine[...] = src(pl.multiple_of(core * hw, LANES), hw)[...] + land[...]
        for t in first:
            t.start()

    def quarters():
        for t, q, p in zip(first, (qa, qb), (0, 1)):
            t.wait()
            q[...] += parts[p]
        for t in second:
            t.start()

    def rest():
        for t, q, p in zip(second, (qa, qb), (2, 3)):
            t.wait()
            q[...] += parts[p]
        back.start()

    def last():
        back.wait()
        theirs_out[...] = theirs[...]

    return give.start, halves, quarters, rest, last


def grad_kernel(coef, feat_coef, sub, d_ff, bias_ref, err_ref, zt_ref, x_ref, hs_ref, lse_ref, norm1_ref, inv1_ref,
                outg_ref, act_ref, pre_ref, normed_ref, norm0_ref, wu_ref, wd_ref, pg_ref,
                out_ref, kl_ref, pm_ref, pt_ref, gm_ref, gt_ref,
                hg_ref, ig_ref, lg_ref, lc, lxa, lyb, lya, lxb, pback, pland, pparts, gback, gland, gparts,
                own_sem, fwd_sem, core_sem, rs_sem, loc_sem, ps_sem, gs_sem):
    k, i = pl.program_id(0), pl.program_id(1)
    n_k, n_i = pl.num_programs(0), pl.num_programs(1)
    dev_x, dev_y, dev_c = neighbours()
    dp, tp = lax.axis_index('dp'), lax.axis_index('tp')
    depth, width = hs_ref.shape
    rows = x_ref.shape[0]
    cut = (depth // 2 + 7) // 8 * 8
    half = rows // 2
    tx = lax.rem(tp + 2, 4)
    own, x_own, y_own, d_own = 2 * tp + dp, 2 * tx + dp, 2 * tp + 1 - dp, 2 * tx + 1 - dp

    def region(owner, c, lo=0, n=None):
        col = pl.multiple_of(owner * (width * n_k) + c * width, LANES)
        return out_ref.at[pl.ds(lo, depth if n is None else n), pl.ds(col, width)]

    def copies(c):
        return [send(hg_ref.at[c], region(own, c), own_sem, (q, c), dev) for q, dev in enumerate((dev_x, dev_y, dev_c))]

    def local(c):
        return pltpu.make_async_copy(hg_ref.at[c], region(own, c), loc_sem.at[c])

    def forward(c):
        return (send(region(x_own, c, 0, cut), region(x_own, c, 0, cut), fwd_sem, (0, c), dev_y),
                send(region(y_own, c, cut, depth - cut), region(y_own, c, cut, depth - cut), fwd_sem, (1, c), dev_x))

    def core(c):
        return [send(r, r, core_sem, (q, c), dev_c) for q, r in enumerate(
            (region(x_own, c), region(y_own, c), region(d_own, c, 0, cut), region(d_own, c, cut, depth - cut)))]

    def serve(c):
        for q in range(2):
            copies(c)[q].wait_recv()
            forward(c)[q].start()
            core(c)[q].start()

    def serve_far(c):
        for q in range(2):
            forward(c)[q].wait_recv()
            core(c)[2 + q].start()

    @pl.when(jnp.logical_and(k == 0, i == 0))
    def _():
        entry_barrier(neighbours())
        kl_ref[...] = jnp.zeros_like(kl_ref)

    devs, me_core = (dev_x, dev_y, dev_c), lax.rem(tp, 2)
    proj_steps = small_sum(lambda col, n: pg_ref.at[:, pl.ds(col, n)], pm_ref, pt_ref, pback, pland, pparts, ps_sem, devs, me_core)
    for at, step in zip((0, 1, 3, 5, 7), proj_steps):
        pl.when(jnp.logical_and(k == 0, i == at))(step)

    tok = pl.ds(pl.multiple_of(i * rows, LANES), rows)
    lse_t, lse_s = lse_ref[:, 0:1], lse_ref[:, 1:2]
    for c in range(0, width, sub):
        z_s = mm(x_ref[...], hs_ref[:, c:c + sub])
        if c + sub == width:
            lane = lax.broadcasted_iota(jnp.int32, (1, sub), 1)
            z_s = z_s + jnp.where(jnp.logical_and(lane >= sub - LANES, k == n_k - 1), bias_ref[0], 0.0)
        log_s = z_s - lse_s
        log_t = zt_ref[:, c:c + sub] - lse_t
        p_t = jnp.exp(log_t)
        lg_ref[:, c:c + sub] = (jnp.exp(log_s) - p_t).astype(BF16)
        kl_ref[0:1, c:c + sub] += jnp.sum(p_t * (log_t - log_s), axis=0, keepdims=True)
    lg = lg_ref[...]
    part_h, part_i = mm_tn(x_ref[...], lg), mm_nt(hs_ref[...], lg)

    @pl.when(i == 0)
    def _():
        hg_ref[k] = part_h

    @pl.when(i > 0)
    def _():
        hg_ref[k] = hg_ref[k] + part_h

    @pl.when(k == 0)
    def _():
        ig_ref[:, tok] = part_i

    @pl.when(k > 0)
    def _():
        ig_ref[:, tok] += part_i

    @pl.when(i == n_i - 1)
    def _():
        hg_ref[k] = hg_ref[k] * coef

    @pl.when(jnp.logical_and(i == n_i - 1, k < n_k - 1))
    def _():
        for t in copies(k):
            t.start()
        local(k).start()

    @pl.when(jnp.logical_and(k == 2, i == 2))
    def _():
        serve(0)

    @pl.when(jnp.logical_and(k == 3, i == 5))
    def _():
        serve(1)

    @pl.when(jnp.logical_and(k == n_k - 1, i == n_i - 1))
    def _():
        def col(r, lo=0, n=rows):
            return ig_ref.at[:, pl.ds(r * rows + lo, n)]

        step0 = [send(col(2 * p + 1), lc.at[p], rs_sem, (p,), dev_c) for p in range(4)]
        step1 = [send(col(4 * d + 2, 0, half), lxa.at[d], rs_sem, (4 + d,), dev_x) for d in range(2)]
        step1 += [send(col(4 + 2 * d, half, half), lyb.at[d], rs_sem, (6 + d,), dev_y) for d in range(2)]
        step2 = [send(col(4, 0, half), lya, rs_sem, (8,), dev_y), send(col(2, half, half), lxb, rs_sem, (9,), dev_x)]
        for t in step0:
            t.start()
        serve(2)
        for p in range(4):
            step0[p].wait_recv()
            col(2 * p)[...] += lc[p]
        for t in step1:
            t.start()
        serve_far(0)
        for t in step1:
            t.wait_recv()
        for d in range(2):
            col(4 * d, 0, half)[...] += lxa[d]
            col(2 * d, half, half)[...] += lyb[d]
        for t in step2:
            t.start()
        for t in copies(4):
            t.start()
        local(4).start()
        serve_far(1)
        serve(3)
        for t in step2:
            t.wait_recv()
        for t in step0 + step1 + step2:
            t.wait_send()
        hig = coef * jnp.concatenate([col(0, 0, half)[...] + lya[...], col(0, half, half)[...] + lxb[...]], axis=1)

        grad_out = outg_ref[...] + hig
        normed1 = norm1_ref[...]
        resid = inv1_ref[...] * (grad_out - normed1 * jnp.mean(grad_out * normed1, axis=0, keepdims=True))
        resid = resid.astype(BF16)
        n_ff = act_ref.shape[0]
        ig_ref[:, n_ff:2 * n_ff] = mm_nt(resid, act_ref[...])
        pre_grad = gelu_back(pre_ref[...], mm(wd_ref[...], resid)).astype(BF16)
        up_grad = mm_nt(normed_ref[...], pre_grad)
        gain = jnp.sum(mm(wu_ref[...], pre_grad) * norm0_ref[...], axis=1, keepdims=True)
        loss = feat_coef * err_ref[0] + coef * jnp.sum(kl_ref[0:1, :])
        lane = lax.broadcasted_iota(jnp.int32, up_grad.shape, 1)
        row0 = lax.broadcasted_iota(jnp.int32, up_grad.shape, 0) == 0
        extra = jnp.where(lane == d_ff, gain, jnp.where(jnp.logical_and(lane == d_ff + 1, row0), loss, 0.0))
        ig_ref[:, :n_ff] = jnp.where(lane < d_ff, up_grad, extra)

        grad_steps = small_sum(lambda col, n: ig_ref.at[:, pl.ds(col, n)], gm_ref, gt_ref, gback, gland, gparts, gs_sem, devs, me_core)
        grad_steps[0]()
        serve(4)
        grad_steps[1]()
        serve_far(2)
        grad_steps[2]()
        serve_far(3)
        grad_steps[3]()
        serve_far(4)
        grad_steps[4]()

        @pl.loop(0, n_k)
        def _(c):
            local(c).wait()
            for t in copies(c):
                t.wait_send()
            copies(c)[2].wait_recv()
            for t in forward(c):
                t.wait_send()
            for t in core(c):
                t.wait()


def grad_pass(zt, x, hs, lse, bias, err, back, n_k, rows, coef, feat_coef, d_ff, n_dev, sub=256):
    n_tok, depth = x.shape
    span = hs.shape[1]
    width = span // n_k
    half = rows // 2
    n_ff, d_proj = back[3].shape[0], back[9].shape[1]
    dma = pltpu.SemaphoreType.DMA
    smem = pl.BlockSpec(memory_space=pltpu.SMEM)

    def whole(shape):
        return pl.BlockSpec(shape, lambda k, i: (0,) * len(shape), pipeline_mode=pl.Buffered(1))

    sums = [(depth, d_proj // 2)] * 2 + [(depth, n_ff)] * 2
    return pl.pallas_call(
        functools.partial(grad_kernel, coef, feat_coef, sub, d_ff),
        grid=(n_k, n_tok // rows),
        in_specs=[smem, smem, pl.BlockSpec((rows, width), lambda k, i: (i, k)),
                  pl.BlockSpec((rows, depth), lambda k, i: (i, 0)),
                  pl.BlockSpec((depth, width), lambda k, i: (0, k)), pl.BlockSpec((rows, LANES), lambda k, i: (i, 0))]
        + [whole(v.shape) for v in back],
        out_specs=[pl.BlockSpec(memory_space=pl.ANY), whole((8, width))] + [whole(v) for v in sums],
        out_shape=[jax.ShapeDtypeStruct((depth, n_dev * span), F32), jax.ShapeDtypeStruct((8, width), F32)]
        + [jax.ShapeDtypeStruct(v, F32) for v in sums],
        scratch_shapes=[pltpu.VMEM((n_k, depth, width), F32), pltpu.VMEM((depth, n_tok), F32), pltpu.VMEM((rows, width), BF16),
                        pltpu.VMEM((4, depth, rows), F32), pltpu.VMEM((2, depth, half), F32), pltpu.VMEM((2, depth, half), F32),
                        pltpu.VMEM((depth, half), F32), pltpu.VMEM((depth, half), F32),
                        pltpu.VMEM((depth, d_proj // 2), F32), pltpu.VMEM((depth, d_proj // 2), F32), pltpu.VMEM((4, depth, d_proj // 4), F32),
                        pltpu.VMEM((depth, n_ff), F32), pltpu.VMEM((depth, n_ff), F32), pltpu.VMEM((4, depth, n_ff // 2), F32),
                        dma((2, 3, n_k)), dma((2, 2, n_k)), dma((2, 4, n_k)), dma((2, 10)), dma((n_k,)), dma((2, 6)), dma((2, 6))],
        compiler_params=pltpu.CompilerParams(dimension_semantics=("arbitrary", "arbitrary"), collective_id=1,
                                             has_side_effects=True, vmem_limit_bytes=62 * 2**20),
        name="grad_pass",
    )(bias, err, zt, x, hs, lse, *back)


UNIT = 256


def teacher_kernel(bias_ref, x_ref, gain_ref, hs_ref, head_ref, tail_ref, wu_ref, wd_ref, rj_ref, xu0, xd0,
                   hid_ref, lse_ref, zt_ref, stud_ref, pu, pd, xu, xd, cxu, cxd, yu, yd, cyu, cyd,
                   lu, ld, n_ref, acc_ref, tile_ref, m_ref, s_ref, mh, sh, w_ref, fl, stage, pk, sl,
                   p_sem, x_sem, cx_sem, y_sem, cy_sem, r_sem, l_sem, t_sem, o_sem, f_sem, z_sem, s_sem, w_sem):
    dev_x, dev_y, dev_c = neighbours()
    dp = lax.axis_index('dp')
    n_layers = wu_ref.shape[0]
    rows = x_ref.shape[0]
    half = wu_ref.shape[2] // 2
    cut = rows // 2

    def col0(h):
        return pl.multiple_of(dp * half + h * UNIT, UNIT)

    def x_send(l, h):
        j = 2 * l + h
        return (send(wu_ref.at[l, :, pl.ds(col0(h), UNIT)], xu.at[j], x_sem, (0, j), dev_x),
                send(wd_ref.at[l, pl.ds(col0(h), UNIT), :], xd.at[j], x_sem, (1, j), dev_x))

    def from_x(j, first):
        return (xu0, xd0) if first else (xu.at[j], xd.at[j])

    def cx_send(j, first=False):
        up, down = from_x(j, first)
        return send(up, cxu.at[j], cx_sem, (0, j), dev_c), send(down, cxd.at[j], cx_sem, (1, j), dev_c)

    def y_send(j, first=False):
        up, down = from_x(j, first)
        return send(up, yu.at[j], y_sem, (0, j), dev_y), send(down, yd.at[j], y_sem, (1, j), dev_y)

    def cy_send(j):
        return send(yu.at[j], cyu.at[j], cy_sem, (0, j), dev_c), send(yd.at[j], cyd.at[j], cy_sem, (1, j), dev_c)

    def p_send(l):
        return (send(wu_ref.at[l], pu.at[l], p_sem, (0, l), dev_c), send(wd_ref.at[l], pd.at[l], p_sem, (1, l), dev_c))

    def slot(r, lo=0, n=None):
        return stud_ref.at[pl.ds(r * rows + lo, rows if n is None else n)]

    r_x = send(rj_ref, slot(2), r_sem, (0,), dev_x)
    r_y = send(rj_ref, slot(4), r_sem, (1,), dev_y)
    r_c = send(rj_ref, slot(1), r_sem, (2,), dev_c)
    r_cx = send(slot(2), slot(3), r_sem, (3,), dev_c)
    r_cy = send(slot(4), slot(5), r_sem, (4,), dev_c)
    r_xy = send(slot(2, 0, cut), slot(6, 0, cut), r_sem, (5,), dev_y)
    r_yx = send(slot(4, cut, rows - cut), slot(6, cut, rows - cut), r_sem, (6,), dev_x)
    r_cd = send(slot(6), slot(7), r_sem, (7,), dev_c)
    r_own = pltpu.make_async_copy(rj_ref, slot(0), o_sem)

    entry_barrier(peers())
    r_x.start()
    r_y.start()
    r_c.start()
    r_own.start()
    for t in y_send(0, True) + cx_send(0, True) + x_send(0, 1) + p_send(0):
        t.start()
    x_send(1, 0)[0].start()

    tp = lax.axis_index('tp')
    shard, span = head_ref.shape[0], w_ref.shape[0]
    shift = pl.multiple_of(tp * (-shard % LANES), -shard % LANES)
    n_in = shard // LANES * LANES - span
    w_first = pltpu.make_async_copy(head_ref.at[pl.ds(shift, span)], w_ref, w_sem.at[0])
    w_second = (pltpu.make_async_copy(head_ref.at[pl.ds(span + shift, n_in)], w_ref.at[pl.ds(0, n_in)], w_sem.at[0]),
                pltpu.make_async_copy(tail_ref.at[pl.ds(shift, span - n_in)], w_ref.at[pl.ds(n_in, span - n_in)], w_sem.at[1]))

    def load_head(act):
        @pl.when(dp == 0)
        def _():
            getattr(w_first, act)()

        @pl.when(dp == 1)
        def _():
            for c in w_second:
                getattr(c, act)()

    load_head('start')
    hid_ref[...] = x_ref[...]
    r_own.wait()

    def x_part(j, part):
        l, h = j // 2, lax.rem(j, 2)
        return x_send(l, h)[part]

    def relay_x(j, part):
        x = x_part(j, part)
        x.wait_recv()
        y_send(j)[part].start()
        cx_send(j)[part].start()
        x.wait_send()

        later = (j + 1, 1) if part == 0 else (j + 2, 0)

        @pl.when(later[0] < 2 * n_layers)
        def _():
            x_part(*later).start()

    def relay_y(j, part):
        y_send(j)[part].wait_recv()
        cy_send(j)[part].start()

    n_col = 5
    width = hs_ref.shape[1] // n_col

    def stud_tile(r):
        load = pltpu.make_async_copy(slot(r), tile_ref, t_sem)
        load.start()
        load.wait()
        m_ref[...] = jnp.full_like(m_ref, NEG)
        s_ref[...] = jnp.zeros_like(s_ref)

        @pl.loop(0, n_col)
        def _(j):
            logit_blocks(tile_ref[...], hs_ref, j * width, width, bias_ref[0], j == n_col - 1, m_ref, s_ref)

        pk[pl.ds(8 + r, 1), :] = lse_row(m_ref, s_ref)

    def load_units(pairs, act):
        for u, (src_u, src_d) in pairs:
            for c in (pltpu.make_async_copy(src_u, lu.at[u], l_sem.at[0, u]), pltpu.make_async_copy(src_d, ld.at[u], l_sem.at[1, u])):
                getattr(c, act)()

    def run_units(lo, hi):
        @pl.loop(lo, hi, step=2)
        def _(u):
            part = None
            for v in range(2):
                p = mm(gelu_tanh(mm(n_ref[...], lu[u + v])).astype(BF16), ld[u + v])
                part = p if part is None else part + p
            acc_ref[...] += part

    cols = [pl.ds(q * UNIT, UNIT) for q in range(4)]

    def own_units(l):
        return [(q, (wu_ref.at[l, :, cols[q]], wd_ref.at[l, cols[q], :])) for q in range(4)]

    def partner_units(l):
        return [(4 + q, (pu.at[l, :, cols[q]], pd.at[l, cols[q], :])) for q in range(4)]

    load_units(own_units(0), 'start')
    stud_tile(0)
    for t in p_send(0):
        t.wait_recv()
    load_units(partner_units(0), 'start')

    @pl.loop(0, n_layers)
    def _(l):
        j0, j1 = 2 * l, 2 * l + 1
        more = l < n_layers - 1

        @pl.when(more)
        def _():
            for t in p_send(l + 1):
                t.start()

        n_ref[...] = (rms_parts(hid_ref[...])[0] * gain_ref[l]).astype(BF16)
        acc_ref[...] = jnp.zeros_like(acc_ref)
        load_units(own_units(l), 'wait')
        run_units(0, 4)

        @pl.when(l == 0)
        def _():
            r_x.wait_recv()
            r_xy.start()
            r_cx.start()
            r_y.wait_recv()
            r_yx.start()
            r_cy.start()
            r_c.wait_recv()

        relay_x(j1, 0)
        relay_y(j0, 0)

        @pl.when(l == 1)
        def _():
            r_xy.wait_recv()
            r_yx.wait_recv()
            r_cd.start()
            r_cx.wait_recv()

        @pl.when(l == 2)
        def _():
            r_cy.wait_recv()
            r_cd.wait_recv()

        for t in cx_send(j0):
            t.wait_recv()
        chip0 = [(8, from_x(j0, False)), (9, (cxu.at[j0], cxd.at[j0]))]

        @pl.when(l == 0)
        def _():
            load_units([(8, from_x(j0, True))], 'start')

        @pl.when(l > 0)
        def _():
            load_units(chip0[:1], 'start')

        load_units(chip0[1:], 'start')
        load_units(partner_units(l), 'wait')
        load_units(chip0, 'wait')
        run_units(4, 10)

        relay_x(j1, 1)
        relay_y(j0, 1)
        stud_tile(2 * l + 1)
        for t in cx_send(j1) + cy_send(j0):
            t.wait_recv()
        chip1 = [(10, (xu.at[j1], xd.at[j1])), (11, (cxu.at[j1], cxd.at[j1])),
                 (12, (yu.at[j0], yd.at[j0])), (13, (cyu.at[j0], cyd.at[j0]))]
        load_units(chip1, 'start')

        @pl.when(more)
        def _():
            load_units(own_units(l + 1), 'start')
            for t in p_send(l + 1):
                t.wait_recv()
            load_units(partner_units(l + 1), 'start')
            relay_x(j1 + 1, 0)

        relay_y(j1, 0)
        load_units(chip1, 'wait')
        run_units(10, 14)

        @pl.when(more)
        def _():
            relay_x(j1 + 1, 1)

        stud_tile(2 * l + 2)
        relay_y(j1, 1)

        @pl.when(jnp.logical_not(more))
        def _():
            stud_tile(7)

        for t in cy_send(j1):
            t.wait_recv()
        chip2 = [(14, (yu.at[j1], yd.at[j1])), (15, (cyu.at[j1], cyd.at[j1]))]
        load_units(chip2, 'start')
        load_units(chip2, 'wait')
        run_units(14, 16)
        hid_ref[...] = hid_ref[...] + acc_ref[...].astype(BF16)

    fl[0] = rms_parts(hid_ref[...])[0].astype(BF16)
    load_head('wait')

    def part(r, h):
        return fl.at[r, pl.ds(h * cut, cut)]

    f_x = [send(part(0, h), part(2, h), f_sem, (h,), dev_x) for h in range(2)]
    f_y = [send(part(0, h), part(4, h), f_sem, (2 + h,), dev_y) for h in range(2)]
    f_c = send(fl.at[0], fl.at[1], f_sem, (4,), dev_c)
    f_cx = [send(part(2, h), part(3, h), f_sem, (5 + h,), dev_c) for h in range(2)]
    f_cy = [send(part(4, h), part(5, h), f_sem, (7 + h,), dev_c) for h in range(2)]
    f_d = [send(part(2, 0), part(6, 0), f_sem, (9,), dev_y), send(part(4, 1), part(6, 1), f_sem, (10,), dev_x)]
    f_cd = [send(part(6, h), part(7, h), f_sem, (11 + h,), dev_c) for h in range(2)]
    for t in (f_x[0], f_y[1], f_c):
        t.start()

    def on_arrival(g, arrived, then):
        @pl.when(g == then[0])
        def _():
            for t in arrived:
                t.wait_recv()
            for t in then[1]:
                t.start()

    @pl.loop(0, 8)
    def _(g):
        on_arrival(g, [f_c], (1, []))
        on_arrival(g, [f_x[0], f_y[1]], (2, [f_cx[0], f_cy[1], f_x[1], f_y[0]]))
        on_arrival(g, [f_cx[0], f_cy[1]], (3, []))
        on_arrival(g, [f_x[1], f_y[0]], (4, [f_d[0], f_d[1], f_cx[1], f_cy[0]]))
        on_arrival(g, [f_cx[1], f_cy[0]], (5, []))
        on_arrival(g, f_d, (6, f_cd))
        on_arrival(g, f_cd, (7, []))
        mixed = jnp.logical_and(g >= 2, g < 6)
        late = jnp.logical_and(g >= 4, g < 6)

        @pl.loop(0, 2)
        def _(u):
            r = g - jnp.where(late, 2, 0) + jnp.where(mixed, 2 * u, 0)
            h = jnp.where(late, 1 - u, u)
            row = pl.multiple_of(h * cut, cut)
            mh[...] = jnp.full_like(mh, NEG)
            sh[...] = jnp.zeros_like(sh)

            @pl.loop(0, n_col)
            def _(j):
                n = (2 * g + u) * n_col + j
                slot_z = lax.rem(n, 2)
                store = pltpu.make_async_copy(stage.at[slot_z], zt_ref.at[pl.ds(pl.multiple_of(r * rows + row, cut), cut),
                                                                          pl.ds(pl.multiple_of(j * width, LANES), width)],
                                              z_sem.at[slot_z])

                @pl.when(n >= 2)
                def _():
                    store.wait()

                logit_blocks(fl[r, pl.ds(row, cut), :], w_ref, j * width, width, bias_ref[0], j == n_col - 1, mh, sh,
                             stage.at[slot_z], by_rows=True)
                store.start()

            pk[pl.ds(r, 1), pl.ds(row, cut)] = lse_row(mh, sh)

    for q in range(2):
        pltpu.make_async_copy(stage.at[q], zt_ref.at[pl.ds(0, cut), pl.ds(0, width)], z_sem.at[q]).wait()

    tell = [send(pk, sl.at[r], s_sem, (r,), dev) for r, dev in zip(range(1, 8), peers())]
    for t in tell:
        t.start()
    sl[0] = pk[...]
    for t in tell:
        t.wait_recv()
    sub = lax.broadcasted_iota(jnp.int32, (LANES, 1), 0)
    for q in range(8):
        both = []
        for base in (0, 8):
            vals = [sl[r, base + (q ^ r):base + (q ^ r) + 1, :] for r in range(8)]
            top = functools.reduce(jnp.maximum, vals)
            both.append(top + jnp.log(sum(jnp.exp(v - top) for v in vals)))
        lse_ref[q * rows:(q + 1) * rows, :] = jnp.where(sub == 0, both[0], jnp.where(sub == 1, both[1], 0.0)).T
    for t in tell + f_x + f_y + f_cx + f_cy + f_d + f_cd + [f_c]:
        t.wait_send()

    for t in (r_x, r_y, r_c, r_cx, r_cy, r_xy, r_yx, r_cd):
        t.wait_send()

    @pl.loop(0, n_layers)
    def _(l):
        for t in p_send(l):
            t.wait_send()
        for h in range(2):
            j = 2 * l + h
            for t in y_send(j) + cx_send(j) + cy_send(j):
                t.wait_send()


def teacher(x, gain, hs, head, tail, w_up, w_down, rj, bias, ahead):
    rows, depth = x.shape
    n_layers, _, shard = w_up.shape
    d_stud, span = hs.shape
    n_ch, cut = 2 * n_layers, rows // 2
    width = span // 5
    any_spec, vmem = pl.BlockSpec(memory_space=pl.ANY), pl.BlockSpec(memory_space=pltpu.VMEM)
    up, down = (n_ch, depth, UNIT), (n_ch, UNIT, depth)
    shapes = [((rows, depth), BF16), ((8 * rows, LANES), F32), ((8 * rows, span), F32), ((8 * rows, d_stud), BF16),
              ((n_layers, depth, shard), BF16), ((n_layers, shard, depth), BF16)]
    shapes += [(s, BF16) for s in (up, down) * 4]
    dma = pltpu.SemaphoreType.DMA
    out = pl.pallas_call(
        teacher_kernel,
        in_specs=[pl.BlockSpec(memory_space=pltpu.SMEM), vmem, vmem, vmem] + [any_spec] * 7,
        out_specs=[vmem, vmem] + [any_spec] * (len(shapes) - 2),
        out_shape=[jax.ShapeDtypeStruct(*s) for s in shapes],
        scratch_shapes=[pltpu.VMEM((16, depth, UNIT), BF16), pltpu.VMEM((16, UNIT, depth), BF16),
                        pltpu.VMEM((rows, depth), BF16), pltpu.VMEM((rows, depth), F32), pltpu.VMEM((rows, d_stud), BF16),
                        pltpu.VMEM((rows, LANES), F32), pltpu.VMEM((rows, LANES), F32),
                        pltpu.VMEM((cut, LANES), F32), pltpu.VMEM((cut, LANES), F32),
                        pltpu.VMEM((span, depth), BF16), pltpu.VMEM((8, rows, depth), BF16),
                        pltpu.VMEM((2, cut, width), F32), pltpu.VMEM((16, rows), F32), pltpu.VMEM((8, 16, rows), F32),
                        dma((2, 2, n_layers))] + [dma((2, 2, n_ch))] * 4
        + [dma((2, 8)), dma((2, 16)), dma, dma, dma((2, 13)), dma((2,)), dma((2, 8)), dma((2,))],
        compiler_params=pltpu.CompilerParams(collective_id=0, has_side_effects=True, vmem_limit_bytes=63 * 2**20),
        name="teacher",
    )(bias, x, gain, hs, head, tail, w_up, w_down, rj, *ahead)
    return out[:4]


def solution(mesh):
    dp_size, tp_size = mesh.shape['dp'], mesh.shape['tp']
    n_dev = dp_size * tp_size

    def local_step(x_teach, x_stud, w_up_t, w_down_t, gain_t, head_t, w_up_s, w_down_s, gain_s, proj_s, head_s):
        dp, tp = lax.axis_index('dp'), lax.axis_index('tp')
        n_b, seq_part, d_teach = x_teach.shape
        own_tok = n_b * seq_part
        n_tok = own_tok * n_dev
        d_stud, vocab = head_s.shape
        n_layers = w_up_t.shape[0]
        seq = x_stud.shape[1]
        blocks = -(-vocab // LANES)
        span = -(-blocks // n_dev) * LANES
        n_chunks = 5
        width = span // n_chunks
        feat_coef = 1.0 / (n_tok * d_teach)
        kl_coef = 1.0 / n_tok

        first = dp * (w_up_t.shape[2] // 2)
        ahead = (swap_x(lax.dynamic_slice_in_dim(w_up_t[0], first, UNIT, axis=1)),
                 swap_x(lax.dynamic_slice_in_dim(w_down_t[0], first, UNIT, axis=0)))

        def seq_rows(other):
            return lax.dynamic_slice_in_dim(x_stud[0], other * seq_part, seq_part, axis=0)

        from_c = swap_core(seq_rows(tp + 1 - 2 * (tp % 2)))
        from_x = swap_x(seq_rows((tp + 2) % 4))
        from_d = lax.ppermute(seq_rows(3 - tp), 'tp', [(i, 3 - i) for i in range(4)])
        mine = seq_rows(tp)
        odd, right = tp % 2 == 1, tp >= 2
        low, high = jnp.where(odd, from_c, mine), jnp.where(odd, mine, from_c)
        far_low, far_high = jnp.where(odd, from_d, from_x), jnp.where(odd, from_x, from_d)
        xs = jnp.concatenate([jnp.where(right, far_low, low), jnp.where(right, far_high, high),
                              jnp.where(right, low, far_low), jnp.where(right, high, far_high)], axis=0)

        owner = 2 * tp + dp
        last = is_last_owner()
        head_rows = head_t.T
        nxt = lax.ppermute(head_rows[:LANES], 'tp', [(1, 0), (2, 1), (3, 2)])
        edge = head_rows.shape[0] // LANES * LANES
        tail = jnp.concatenate([head_rows[edge:], nxt], axis=0)
        over = n_dev * span - vocab
        my_hs = lax.dynamic_slice_in_dim(head_s, pl.multiple_of(owner * span - jnp.where(last, over, 0), LANES), span, axis=1)
        my_hs = jnp.where(last, jnp.pad(my_hs[:, over:], ((0, 0), (0, over))), my_hs)
        bias = jnp.where(last, NEG, 0.0).astype(F32).reshape(1)

        d_ff = w_up_s.shape[2]
        pad_ff = -d_ff % LANES
        up_s = jnp.pad(w_up_s[0], ((0, 0), (0, pad_ff)))
        down_s = jnp.pad(w_down_s[0], ((0, pad_ff), (0, 0)))
        resid0 = xs.T.astype(F32)
        norm0, _ = rms_parts(resid0, 0)
        normed_s = (norm0 * gain_s[0][:, None]).astype(BF16)
        pre_act = mm_tn(up_s, normed_s)
        act_s = gelu_tanh(pre_act).astype(BF16)
        norm1, inv1 = rms_parts(resid0 + mm_tn(down_s, act_s), 0)
        proj_in = norm1.T.astype(BF16)

        hidden, lse, zt, stud_full = teacher(x_teach.reshape(own_tok, d_teach), gain_t, my_hs, head_rows, tail, w_up_t, w_down_t,
                                             proj_in, bias, ahead)

        feat_err = mm(proj_in, proj_s[0]) - hidden.astype(F32)
        err_total = jnp.sum(feat_err * feat_err)
        err_grad = (2.0 * feat_coef * feat_err).astype(BF16)
        proj_grad = mm_tn(proj_in, err_grad)
        out_grad = mm_nt(proj_s[0], err_grad)

        back = (norm1, inv1, out_grad, act_s, pre_act, normed_s, norm0, up_s, down_s, proj_grad)
        head_grad, _, proj_a, proj_b, ff_a, ff_b = grad_pass(
            zt, stud_full, my_hs, lse, bias, err_total.reshape(1), back, n_chunks, own_tok, kl_coef, feat_coef, d_ff, n_dev)
        low = tp % 2 == 0
        grad_proj = jnp.where(low, jnp.concatenate([proj_a, proj_b], axis=1), jnp.concatenate([proj_b, proj_a], axis=1))[None]
        first, second = jnp.where(low, ff_a, ff_b), jnp.where(low, ff_b, ff_a)
        grad_up = first[:, :d_ff][None]
        grad_gain = first[:, d_ff][None]
        total_loss = first[0, d_ff + 1]
        grad_down = second[:, :d_ff].T[None]
        head_grad = head_grad[:, :vocab]
        return total_loss, grad_up, grad_down, grad_gain, grad_proj, head_grad

    in_specs = (P('dp', 'tp', None), P(('dp', 'tp'), None, None), P(None, None, 'tp'), P(None, 'tp', None),
                P(), P(None, 'tp'), P(), P(), P(), P(), P())
    out_specs = (P(), P(), P(), P(), P(), P())
    return jax.shard_map(local_step, mesh=mesh, in_specs=in_specs, out_specs=out_specs, check_vma=False)
```
